32 devices in a mesh: fld: 2 (over x), col: 4 (over z), row: 4 (over y, core).
Axes of the slice: x: 2, y: 2, z: 4, core: 2. Of those that a mesh axis runs over, the one named last changes fastest.
Arguments:
- u_real: float32 [32, 128, 128, 128], P('fld', None, 'row', 'col'), parts along dimension 0
- u_imag: float32 [32, 128, 128, 128], P('fld', None, 'row', 'col'), parts along dimension 0
- g_filter: float32 [128, 128, 128], P('row', 'col')
Outputs:
- output 1: float32 [32, 128, 128, 128], P('fld', 'row', 'col'), parts along dimension 0
- output 2: float32 [32, 128, 128, 128], P('fld', 'row', 'col'), parts along dimension 0
There are 2 independent parts. The reference program is written for one: setup_inputs(seed, part) draws one part's arguments, and reference() takes and returns one part's arrays. A program takes and returns all parts, laid end to end along the dimension named above; an argument that names none is the same for every part.
All inputs are finite; a program needn't handle non-finite values.
Results may differ from the reference program's by a relative error of at most 0.001.
Values are sent between devices in bfloat16 or wider.
A program may use at most 1 GiB of HBM per device.

```python
import jax
import jax.numpy as jnp
from jax import lax

N = 128
BATCH = 16


def setup_inputs(seed: int = 0, part: int = 0) -> dict:
    root_key = jax.random.key(seed)
    field_key = jax.random.fold_in(jax.random.fold_in(root_key, 1), part)
    key_re, key_im = jax.random.split(field_key)
    u_real = jax.random.normal(key_re, (BATCH, N, N, N), jnp.float32)
    u_imag = jax.random.normal(key_im, (BATCH, N, N, N), jnp.float32)
    wave_num = ((jnp.arange(N) + N // 2) % N - N // 2).astype(jnp.float32)
    wave_sq = wave_num * wave_num
    k_sq = wave_sq[:, None, None] + wave_sq[None, :, None] + wave_sq[None, None, :]
    profile = 2.0 / (1.0 + 16.0 * k_sq / (N * N))
    jitter = jax.random.uniform(jax.random.fold_in(root_key, 2), (N, N, N), jnp.float32)
    g_filter = profile * (0.5 + jitter)
    return {"u_real": u_real, "u_imag": u_imag, "g_filter": g_filter}


def reference(u_real, u_imag, g_filter):
    def one_field(field_pair):
        field_re, field_im = field_pair
        spectrum = jnp.fft.fftn(field_re + 1j * field_im, norm="ortho")
        filtered = spectrum * g_filter
        return jnp.real(filtered).astype(jnp.float32), jnp.imag(filtered).astype(jnp.float32)
    w_real, w_imag = lax.map(one_field, (u_real, u_imag))
    return w_real, w_imag
```

```python
import functools
import math

import jax
import jax.numpy as jnp
import numpy as np
from jax import lax
from jax.experimental import pallas as pl
from jax.experimental.pallas import tpu as pltpu
from jax.sharding import PartitionSpec as P

MESH = pl.DeviceIdType.MESH
N = 128
B = 32
NP = 4
FG = 4
KC = 8
NJ = B // KC
MSG = 2 * KC * B
SC = 16
TINY = 2.0 ** -126


def dft_tables():
    idx = np.arange(N)
    ang = 2.0 * np.pi * ((idx[:, None] * idx[None, :]) % N) / N
    cos, sin = np.cos(ang) / math.sqrt(N), np.sin(ang) / math.sqrt(N)
    mat = np.stack([np.stack([cos, sin], 1), np.stack([-sin, cos], 1)])
    fx = mat.reshape(2, NP, NJ, KC, 2 * N).transpose(1, 2, 0, 3, 4).reshape(2 * N, 2 * N)
    fy = mat.reshape(2, NP, B, 2, NP, B).transpose(1, 0, 2, 4, 3, 5).reshape(2 * N, 2 * N)
    fz = mat.transpose(2, 3, 0, 1).reshape(2 * N, 2 * N)
    return fx.astype(np.float32), fy.astype(np.float32), fz.astype(np.float32)


def encode(x, scale):
    v = x * (1.0 / scale)
    p = v * v
    p = p * p
    p = p * p
    return jnp.where(v < 0, -p, p).astype(jnp.bfloat16)


def decode(code, scale):
    y = code.astype(jnp.float32)
    p = jnp.maximum(jnp.abs(y), TINY)
    root = lax.rsqrt(lax.rsqrt(p * lax.rsqrt(p)))
    return jnp.where(y < 0, -root, root) * scale


def scale_of(peak):
    return jnp.maximum(peak * 2.0 ** -15, TINY).astype(jnp.bfloat16).astype(jnp.float32)


def kernel(ng, fx_ref, fy_ref, fz_ref, g_ref, ur_ref, ui_ref, wr_ref, wi_ref,
           stage, xsend, xrecv, ysend, yrecv, scales, ostage,
           in_sem, xs_sem, xr_sem, ys_sem, yr_sem, out_sem):
    nt = ng * NJ
    col, row = lax.axis_index("col"), lax.axis_index("row")
    highest = lax.Precision.HIGHEST

    def peer(me, d):
        return lax.rem(me + d, NP)

    def load(grp, slot):
        copies = []
        for c, src in enumerate((ur_ref, ui_ref)):
            copies.append(pltpu.make_async_copy(src.at[pl.ds(grp * FG, FG)], stage.at[slot, c], in_sem.at[slot, c]))
        return copies

    def row_copy(t, d):
        dst = peer(row, d)
        base = pl.multiple_of((lax.rem(t, 2 * NJ) // NJ * NP * NJ + dst * NJ + lax.rem(t, NJ)) * MSG, MSG)
        src = xsend.at[pl.ds(base, MSG)]
        if d == 0:
            return pltpu.make_async_copy(src, xrecv.at[t, row], xr_sem.at[t, row])
        return pltpu.make_async_remote_copy(
            src, xrecv.at[t, row], xs_sem.at[lax.rem(t, 2 * NJ), d], xr_sem.at[t, row],
            device_id={"row": dst}, device_id_type=MESH)

    def col_copy(t, d):
        dst = peer(col, d)
        src = ysend.at[lax.rem(t, 4), dst]
        if d == 0:
            return pltpu.make_async_copy(src, yrecv.at[t, col], yr_sem.at[t, col])
        return pltpu.make_async_remote_copy(
            src, yrecv.at[t, col], ys_sem.at[lax.rem(t, 4), d], yr_sem.at[t, col],
            device_id={"col": dst}, device_id_type=MESH)

    def arrived(buf, sem, t):
        for p in range(NP):
            pltpu.make_async_copy(buf.at[t, p], buf.at[t, p], sem.at[t, p]).wait()

    def x_step(grp):
        slot = lax.rem(grp, 2)
        for copy in load(grp, slot):
            copy.wait()

        def body(yy, _):
            pieces = []
            for dy in range(2):
                y = yy * 2 + dy
                halves = [stage[slot, c, :, pl.ds(y, 1)].reshape(FG * B, N) for c in range(2)]
                pieces.append(jnp.concatenate(halves, axis=1))
            data = jnp.concatenate(pieces, axis=0)
            out = lax.dot_general(fx_ref[...], data, (((1,), (1,)), ((), ())), precision=highest,
                                  preferred_element_type=jnp.float32)
            for dy in range(2):
                for blk in range(2 * NP * NJ):
                    base = slot * (NP * NJ * MSG) + (blk // 2) * MSG + (blk % 2) * B + yy * 2 + dy
                    xsend[pl.ds(base, KC, stride=2 * B), :] = out[blk * KC:(blk + 1) * KC, dy * N:(dy + 1) * N]
            return 0

        lax.fori_loop(0, B // 2, body, 0)

        def send(j, _):
            for d in (2, 1, 3, 0):
                row_copy(grp * NJ + j, d).start()
            return 0

        lax.fori_loop(0, NJ, send, 0)

    def row_drained(grp):
        def body(j, _):
            for d in (1, 2, 3):
                row_copy(grp * NJ + j, d).wait_send()
            return 0

        lax.fori_loop(0, NJ, body, 0)

    def y_step(t):
        slot = lax.rem(t, 4)
        arrived(xrecv, xr_sem, t)

        def body(kk, _):
            cols = []
            for dk in range(2):
                k = kk * 2 + dk
                rows = pl.ds(pl.multiple_of(k * 2 * B, 2 * B), 2 * B)
                cols.append(jnp.concatenate([xrecv[t, p, rows, :] for p in range(NP)], axis=0))
            data = jnp.concatenate(cols, axis=1)
            out = jnp.dot(fy_ref[...], data, precision=highest, preferred_element_type=jnp.float32)
            scale = scale_of(jnp.max(jnp.abs(out), axis=0, keepdims=True))
            out = encode(out, scale)
            for dk in range(2):
                scales[pl.ds(kk * 2 + dk, 1), :] = scale[:, dk * N:(dk + 1) * N]
                for s in range(NP):
                    for c in range(2):
                        rows = pl.ds(pl.multiple_of(c * KC * B + (kk * 2 + dk) * B, B), B)
                        ysend[slot, s, rows, :] = out[(s * 2 + c) * B:(s * 2 + c + 1) * B, dk * N:(dk + 1) * N]
            return 0

        lax.fori_loop(0, KC // 2, body, 0)
        tail = jnp.concatenate([scales[...]] * (SC // KC), axis=0).astype(jnp.bfloat16)
        for s in range(NP):
            ysend[slot, s, MSG:MSG + SC, :] = tail
        for d in (2, 3, 1, 0):
            col_copy(t, d).start()

    def out_copies(t):
        slot = lax.rem(t, 2)
        grp, j = t // NJ, lax.rem(t, NJ)
        return [pltpu.make_async_copy(
            ostage.at[slot, c], dst.at[pl.ds(grp * FG, FG), pl.ds(j * KC, KC)], out_sem.at[slot, c])
            for c, dst in enumerate((wr_ref, wi_ref))]

    def z_step(t):
        slot, j = lax.rem(t, 2), lax.rem(t, NJ)
        arrived(yrecv, yr_sem, t)
        half = KC * B
        gain = g_ref[pl.ds(j * KC, KC)].reshape(half, N)
        group = lax.broadcasted_iota(jnp.int32, (MSG + SC, N), 1) // B
        for f in range(FG):
            code = None
            for q in range(NP):
                piece = yrecv[t, q]
                if q != f:
                    piece = pltpu.roll(piece, (q - f) % NP * B, 1)
                code = piece if code is None else jnp.where(group == q, piece, code)
            rows = code[MSG:].astype(jnp.float32)
            scale = jnp.concatenate([jnp.broadcast_to(rows[k:k + 1], (B, N)) for k in range(KC)], axis=0)
            data = jnp.concatenate([decode(code[c * half:(c + 1) * half], scale) for c in range(2)], axis=1)
            out = jnp.dot(data, fz_ref[...], precision=highest, preferred_element_type=jnp.float32)
            for c in range(2):
                ostage[slot, c, f] = (out[:, c * N:(c + 1) * N] * gain).reshape(KC, B, N)
        for copy in out_copies(t):
            copy.start()

    for grp in range(min(2, ng)):
        for copy in load(grp, grp):
            copy.start()

    barrier = pltpu.get_barrier_semaphore()
    for d in range(1, NP):
        pl.semaphore_signal(barrier, inc=1, device_id={"row": peer(row, d)}, device_id_type=MESH)
        pl.semaphore_signal(barrier, inc=1, device_id={"col": peer(col, d)}, device_id_type=MESH)
    pl.semaphore_wait(barrier, 2 * (NP - 1))

    x_step(0)

    if ng > 1:
        x_step(1)
    if ng > 2:
        for copy in load(2, 0):
            copy.start()

    def tick(t, _):
        @pl.when(t >= 4)
        def _():
            for d in (1, 2, 3):
                col_copy(t - 4, d).wait_send()

        y_step(t)

        @pl.when(t >= 1)
        def _():
            @pl.when(t >= 3)
            def _():
                for copy in out_copies(t - 3):
                    copy.wait()

            z_step(t - 1)

        if ng > 2:
            @pl.when((lax.rem(t, NJ) == NJ - 1) & (t < (ng - 2) * NJ))
            def _():
                grp = t // NJ
                row_drained(grp)
                x_step(grp + 2)

                @pl.when(grp + 3 < ng)
                def _():
                    for copy in load(grp + 3, lax.rem(grp + 3, 2)):
                        copy.start()

        return 0

    lax.fori_loop(0, nt, tick, 0)

    for copy in out_copies(nt - 3):
        copy.wait()
    z_step(nt - 1)
    for t in (nt - 2, nt - 1):
        for copy in out_copies(t):
            copy.wait()
    for grp in range(max(ng - 2, 0), ng):
        row_drained(grp)
    for t in range(nt - 4, nt):
        for d in (1, 2, 3):
            col_copy(t, d).wait_send()


def solution(mesh):
    fx, fy, fz = dft_tables()

    def local_forward(u_real, u_imag, g_filter):
        ng = u_real.shape[0] // FG
        nt = ng * NJ
        u_real, u_imag = (jnp.transpose(u, (0, 2, 3, 1)) for u in (u_real, u_imag))
        out = jax.ShapeDtypeStruct((ng * FG, B, B, N), jnp.float32)
        vmem, anywhere = pl.BlockSpec(memory_space=pltpu.VMEM), pl.BlockSpec(memory_space=pl.ANY)
        flops = 2 * 2 * N * 2 * N * N * B * B // N * ng * FG * 24
        return pl.pallas_call(
            functools.partial(kernel, ng),
            out_shape=(out, out),
            in_specs=[vmem] * 4 + [anywhere] * 2,
            out_specs=(anywhere, anywhere),
            scratch_shapes=[
                pltpu.VMEM((2, 2, FG, B, B, N), jnp.float32),
                pltpu.VMEM((2 * NP * NJ * MSG, N), jnp.float32),
                pltpu.VMEM((nt, NP, MSG, N), jnp.float32),
                pltpu.VMEM((4, NP, MSG + SC, N), jnp.bfloat16),
                pltpu.VMEM((nt, NP, MSG + SC, N), jnp.bfloat16),
                pltpu.VMEM((KC, N), jnp.float32),
                pltpu.VMEM((2, 2, FG, KC, B, N), jnp.float32),
                pltpu.SemaphoreType.DMA((2, 2)),
                pltpu.SemaphoreType.DMA((2 * NJ, NP)),
                pltpu.SemaphoreType.DMA((nt, NP)),
                pltpu.SemaphoreType.DMA((4, NP)),
                pltpu.SemaphoreType.DMA((nt, NP)),
                pltpu.SemaphoreType.DMA((2, 2)),
            ],
            compiler_params=pltpu.CompilerParams(
                collective_id=0, has_side_effects=True, vmem_limit_bytes=67043328),
            cost_estimate=pl.CostEstimate(flops=flops, bytes_accessed=1 << 25, transcendentals=0),
        )(jnp.asarray(fx), jnp.asarray(fy), jnp.asarray(fz), g_filter, u_real, u_imag)

    field_spec = P("fld", None, "row", "col")
    out_spec = P("fld", "row", "col", None)
    return jax.shard_map(local_forward, mesh=mesh, in_specs=(field_spec, field_spec, P("row", "col", None)),
                         out_specs=(out_spec, out_spec), check_vma=False)
```

```python
import functools
import math

import jax
import jax.numpy as jnp
import numpy as np
from jax import lax
from jax.experimental import pallas as pl
from jax.experimental.pallas import tpu as pltpu
from jax.sharding import PartitionSpec as P

MESH = pl.DeviceIdType.MESH
N = 128
B = 32
NP = 4
FG = 4
KC = 8
NJ = B // KC
MSG = 2 * KC * B
SC = 16
TINY = 2.0 ** -126


def dft_tables():
    idx = np.arange(N)
    ang = 2.0 * np.pi * ((idx[:, None] * idx[None, :]) % N) / N
    cos, sin = np.cos(ang) / math.sqrt(N), np.sin(ang) / math.sqrt(N)
    mat = np.stack([np.stack([cos, sin], 1), np.stack([-sin, cos], 1)])
    fx = mat.reshape(2, NP, NJ, KC, 2 * N).transpose(1, 2, 0, 3, 4).reshape(2 * N, 2 * N)
    fy = mat.reshape(2, NP, B, 2, NP, B).transpose(1, 0, 2, 4, 3, 5).reshape(2 * N, 2 * N)
    fz = mat.transpose(2, 3, 0, 1).reshape(2 * N, 2 * N)
    return fx.astype(np.float32), fy.astype(np.float32), fz.astype(np.float32)


def encode(x, scale):
    v = x * (1.0 / scale)
    p = v * v
    p = p * p
    p = p * p
    return jnp.where(v < 0, -p, p).astype(jnp.bfloat16)


def decode(code, scale):
    y = code.astype(jnp.float32)
    p = jnp.maximum(jnp.abs(y), TINY)
    root = lax.rsqrt(lax.rsqrt(p * lax.rsqrt(p)))
    return jnp.where(y < 0, -root, root) * scale


def scale_of(peak):
    return jnp.maximum(peak * 2.0 ** -15, TINY).astype(jnp.bfloat16).astype(jnp.float32)


def kernel(ng, fx_ref, fy_ref, fz_ref, g_ref, ur_ref, ui_ref, wr_ref, wi_ref,
           stage, xout, xsend, xrecv, ysend, yrecv, scales,
           in_sem, xs_sem, xr_sem, ys_sem, yr_sem):
    nt = ng * NJ
    col, row = lax.axis_index("col"), lax.axis_index("row")
    highest = lax.Precision.HIGHEST

    def peer(me, d):
        return lax.rem(me + d, NP)

    def load(grp, slot):
        copies = []
        for c, src in enumerate((ur_ref, ui_ref)):
            copies.append(pltpu.make_async_copy(src.at[pl.ds(grp * FG, FG)], stage.at[slot, c], in_sem.at[slot, c]))
        return copies

    def row_copy(t, d):
        dst = peer(row, d)
        src = xsend.at[lax.rem(t, 2 * NJ), dst]
        if d == 0:
            return pltpu.make_async_copy(src, xrecv.at[t, row], xr_sem.at[t, row])
        return pltpu.make_async_remote_copy(
            src, xrecv.at[t, row], xs_sem.at[lax.rem(t, 2 * NJ), d], xr_sem.at[t, row],
            device_id={"row": dst}, device_id_type=MESH)

    def col_copy(t, d):
        dst = peer(col, d)
        src = ysend.at[lax.rem(t, 4), dst]
        if d == 0:
            return pltpu.make_async_copy(src, yrecv.at[t, col], yr_sem.at[t, col])
        return pltpu.make_async_remote_copy(
            src, yrecv.at[t, col], ys_sem.at[lax.rem(t, 4), d], yr_sem.at[t, col],
            device_id={"col": dst}, device_id_type=MESH)

    def arrived(buf, sem, t):
        for p in range(NP):
            pltpu.make_async_copy(buf.at[t, p], buf.at[t, p], sem.at[t, p]).wait()

    def x_step(grp):
        slot = lax.rem(grp, 2)
        for copy in load(grp, slot):
            copy.wait()

        def body(yy, peak):
            pieces = []
            for dy in range(2):
                y = yy * 2 + dy
                halves = [stage[slot, c, :, pl.ds(y, 1)].reshape(FG * B, N) for c in range(2)]
                pieces.append(jnp.concatenate(halves, axis=1))
            data = jnp.concatenate(pieces, axis=0)
            out = lax.dot_general(fx_ref[...], data, (((1,), (1,)), ((), ())), precision=highest,
                                  preferred_element_type=jnp.float32)
            for dy in range(2):
                for blk in range(2 * NP * NJ):
                    base = blk // 2 * MSG + blk % 2 * B + yy * 2 + dy
                    xout[pl.ds(base, KC, stride=2 * B), :] = out[blk * KC:(blk + 1) * KC, dy * N:(dy + 1) * N]
            tall = jnp.max(jnp.abs(out).reshape(2 * N // 8, 8, 2 * N), axis=0)
            return jnp.maximum(peak, jnp.maximum(tall[:, :N], tall[:, N:]))

        peak = lax.fori_loop(0, B // 2, body, jnp.zeros((8, N), jnp.float32))
        scale = scale_of(jnp.max(peak, axis=0, keepdims=True))
        tail = jnp.broadcast_to(scale, (SC, N)).astype(jnp.bfloat16)

        def send(j, _):
            t = grp * NJ + j
            place = lax.rem(t, 2 * NJ)

            def pack(r, _):
                rows = pl.ds(pl.multiple_of((r * NJ + j) * MSG, MSG), MSG)
                xsend[place, r, :MSG, :] = encode(xout[rows, :], scale)
                xsend[place, r, MSG:, :] = tail
                return 0

            lax.fori_loop(0, NP, pack, 0)
            for d in (2, 1, 3, 0):
                row_copy(t, d).start()
            return 0

        lax.fori_loop(0, NJ, send, 0)

    def row_drained(grp):
        def body(j, _):
            for d in (1, 2, 3):
                row_copy(grp * NJ + j, d).wait_send()
            return 0

        lax.fori_loop(0, NJ, body, 0)

    def y_step(t):
        slot = lax.rem(t, 4)
        arrived(xrecv, xr_sem, t)

        def body(kk, _):
            cols = []
            for dk in range(2):
                k = kk * 2 + dk
                rows = pl.ds(pl.multiple_of(k * 2 * B, 2 * B), 2 * B)
                cols.append(jnp.concatenate(
                    [decode(xrecv[t, p, rows, :], xrecv[t, p, MSG:, :].astype(jnp.float32)[:1]) for p in range(NP)],
                    axis=0))
            data = jnp.concatenate(cols, axis=1)
            out = jnp.dot(fy_ref[...], data, precision=highest, preferred_element_type=jnp.float32)
            scale = scale_of(jnp.max(jnp.abs(out), axis=0, keepdims=True))
            out = encode(out, scale)
            for dk in range(2):
                scales[pl.ds(kk * 2 + dk, 1), :] = scale[:, dk * N:(dk + 1) * N]
                for s in range(NP):
                    for c in range(2):
                        rows = pl.ds(pl.multiple_of(c * KC * B + (kk * 2 + dk) * B, B), B)
                        ysend[slot, s, rows, :] = out[(s * 2 + c) * B:(s * 2 + c + 1) * B, dk * N:(dk + 1) * N]
            return 0

        lax.fori_loop(0, KC // 2, body, 0)
        tail = jnp.concatenate([scales[...]] * (SC // KC), axis=0).astype(jnp.bfloat16)
        for s in range(NP):
            ysend[slot, s, MSG:MSG + SC, :] = tail
        for d in (2, 3, 1, 0):
            col_copy(t, d).start()

    def z_step(t):
        grp, j = t // NJ, lax.rem(t, NJ)
        arrived(yrecv, yr_sem, t)
        half = KC * B
        gain = g_ref[pl.ds(j * KC, KC)].reshape(half, N)
        group = lax.broadcasted_iota(jnp.int32, (MSG + SC, N), 1) // B
        for f in range(FG):
            code = None
            for q in range(NP):
                piece = yrecv[t, q]
                if q != f:
                    piece = pltpu.roll(piece, (q - f) % NP * B, 1)
                code = piece if code is None else jnp.where(group == q, piece, code)
            rows = code[MSG:].astype(jnp.float32)
            scale = jnp.concatenate([jnp.broadcast_to(rows[k:k + 1], (B, N)) for k in range(KC)], axis=0)
            data = jnp.concatenate([decode(code[c * half:(c + 1) * half], scale) for c in range(2)], axis=1)
            out = jnp.dot(data, fz_ref[...], precision=highest, preferred_element_type=jnp.float32)
            for c, dst in enumerate((wr_ref, wi_ref)):
                dst[grp * FG + f, pl.ds(j * KC, KC)] = (out[:, c * N:(c + 1) * N] * gain).reshape(KC, B, N)

    for grp in range(min(2, ng)):
        for copy in load(grp, grp):
            copy.start()

    barrier = pltpu.get_barrier_semaphore()
    for d in range(1, NP):
        pl.semaphore_signal(barrier, inc=1, device_id={"row": peer(row, d)}, device_id_type=MESH)
        pl.semaphore_signal(barrier, inc=1, device_id={"col": peer(col, d)}, device_id_type=MESH)
    pl.semaphore_wait(barrier, 2 * (NP - 1))

    x_step(0)

    if ng > 1:
        x_step(1)
    if ng > 2:
        for copy in load(2, 0):
            copy.start()

    def tick(t, _):
        @pl.when(t >= 4)
        def _():
            for d in (1, 2, 3):
                col_copy(t - 4, d).wait_send()

        y_step(t)

        @pl.when(t >= 1)
        def _():
            z_step(t - 1)

        if ng > 2:
            @pl.when((lax.rem(t, NJ) == NJ - 1) & (t < (ng - 2) * NJ))
            def _():
                grp = t // NJ
                row_drained(grp)
                x_step(grp + 2)

                @pl.when(grp + 3 < ng)
                def _():
                    for copy in load(grp + 3, lax.rem(grp + 3, 2)):
                        copy.start()

        return 0

    lax.fori_loop(0, nt, tick, 0)

    z_step(nt - 1)
    for grp in range(max(ng - 2, 0), ng):
        row_drained(grp)
    for t in range(nt - 4, nt):
        for d in (1, 2, 3):
            col_copy(t, d).wait_send()


def solution(mesh):
    fx, fy, fz = dft_tables()

    def local_forward(u_real, u_imag, g_filter):
        ng = u_real.shape[0] // FG
        nt = ng * NJ
        u_real, u_imag = (jnp.transpose(u, (0, 2, 3, 1)) for u in (u_real, u_imag))
        out = pltpu.VMEM((ng * FG, B, B, N), jnp.float32)
        vmem, anywhere = pl.BlockSpec(memory_space=pltpu.VMEM), pl.BlockSpec(memory_space=pl.ANY)
        flops = 2 * 2 * N * 2 * N * N * B * B // N * ng * FG * 24
        return pl.pallas_call(
            functools.partial(kernel, ng),
            out_shape=(out, out),
            in_specs=[vmem] * 4 + [anywhere] * 2,
            out_specs=(vmem, vmem),
            scratch_shapes=[
                pltpu.VMEM((2, 2, FG, B, B, N), jnp.float32),
                pltpu.VMEM((NP * NJ * MSG, N), jnp.float32),
                pltpu.VMEM((2 * NJ, NP, MSG + SC, N), jnp.bfloat16),
                pltpu.VMEM((nt, NP, MSG + SC, N), jnp.bfloat16),
                pltpu.VMEM((4, NP, MSG + SC, N), jnp.bfloat16),
                pltpu.VMEM((nt, NP, MSG + SC, N), jnp.bfloat16),
                pltpu.VMEM((KC, N), jnp.float32),
                pltpu.SemaphoreType.DMA((2, 2)),
                pltpu.SemaphoreType.DMA((2 * NJ, NP)),
                pltpu.SemaphoreType.DMA((nt, NP)),
                pltpu.SemaphoreType.DMA((4, NP)),
                pltpu.SemaphoreType.DMA((nt, NP)),
            ],
            compiler_params=pltpu.CompilerParams(
                collective_id=0, has_side_effects=True, vmem_limit_bytes=40 << 20),
            cost_estimate=pl.CostEstimate(flops=flops, bytes_accessed=1 << 25, transcendentals=0),
        )(jnp.asarray(fx), jnp.asarray(fy), jnp.asarray(fz), g_filter, u_real, u_imag)

    field_spec = P("fld", None, "row", "col")
    out_spec = P("fld", "row", "col", None)
    return jax.shard_map(local_forward, mesh=mesh, in_specs=(field_spec, field_spec, P("row", "col", None)),
                         out_specs=(out_spec, out_spec), check_vma=False)
```

```python
import functools
import math

import jax
import jax.numpy as jnp
import numpy as np
from jax import lax
from jax.experimental import pallas as pl
from jax.experimental.pallas import tpu as pltpu
from jax.sharding import PartitionSpec as P

MESH = pl.DeviceIdType.MESH
N = 128
B = 32
NP = 4
FG = 4
KC = 8
NJ = B // KC
MSG = 2 * KC * B
SC = 16
TINY = 2.0 ** -126
LAG = 6
YS = LAG + 2


def dft_tables():
    idx = np.arange(N)
    ang = 2.0 * np.pi * ((idx[:, None] * idx[None, :]) % N) / N
    cos, sin = np.cos(ang) / math.sqrt(N), np.sin(ang) / math.sqrt(N)
    mat = np.stack([np.stack([cos, sin], 1), np.stack([-sin, cos], 1)])
    fx = mat.reshape(2, NP, NJ, KC, 2 * N).transpose(1, 2, 0, 3, 4).reshape(2 * N, 2 * N)
    fy = mat.reshape(2, NP, B, 2, NP, B).transpose(1, 0, 2, 4, 3, 5).reshape(2 * N, 2 * N)
    fz = mat.transpose(2, 3, 0, 1).reshape(2 * N, 2 * N)
    return fx.astype(np.float32), fy.astype(np.float32), fz.astype(np.float32)


def encode(x, scale):
    v = x * (1.0 / scale)
    p = v * v
    p = p * p
    p = p * p
    return jnp.where(v < 0, -p, p).astype(jnp.bfloat16)


def decode(code, scale):
    y = code.astype(jnp.float32)
    p = jnp.maximum(jnp.abs(y), TINY)
    root = lax.rsqrt(lax.rsqrt(p * lax.rsqrt(p)))
    return jnp.where(y < 0, -root, root) * scale


def scale_of(peak):
    return jnp.maximum(peak * 2.0 ** -15, TINY).astype(jnp.bfloat16).astype(jnp.float32)


def kernel(ng, fx_ref, fy_ref, fz_ref, g_ref, ur_ref, ui_ref, wr_ref, wi_ref,
           stage, xout, xsend, xrecv, ysend, yrecv, scales,
           in_sem, xs_sem, xr_sem, ys_sem, yr_sem):
    nt = ng * NJ
    col, row = lax.axis_index("col"), lax.axis_index("row")
    highest = lax.Precision.HIGHEST

    def peer(me, d):
        return (me, me + 1 - 2 * lax.rem(me, 2), lax.rem(me + 2, NP), NP - 1 - me)[d]

    def load(grp, slot):
        copies = []
        for c, src in enumerate((ur_ref, ui_ref)):
            copies.append(pltpu.make_async_copy(src.at[pl.ds(grp * FG, FG)], stage.at[slot, c], in_sem.at[slot, c]))
        return copies

    def row_copy(t, d):
        dst = peer(row, d)
        src = xsend.at[lax.rem(t, 2 * NJ), dst]
        if d == 0:
            return pltpu.make_async_copy(src, xrecv.at[t, row], xr_sem.at[t, row])
        return pltpu.make_async_remote_copy(
            src, xrecv.at[t, row], xs_sem.at[lax.rem(t, 2 * NJ), d], xr_sem.at[t, row],
            device_id={"row": dst}, device_id_type=MESH)

    def col_copy(t, d):
        dst = peer(col, d)
        src = ysend.at[lax.rem(t, YS), dst]
        if d == 0:
            return pltpu.make_async_copy(src, yrecv.at[t, col], yr_sem.at[t, col])
        return pltpu.make_async_remote_copy(
            src, yrecv.at[t, col], ys_sem.at[lax.rem(t, YS), d], yr_sem.at[t, col],
            device_id={"col": dst}, device_id_type=MESH)

    def arrived(buf, sem, t):
        for p in range(NP):
            pltpu.make_async_copy(buf.at[t, p], buf.at[t, p], sem.at[t, p]).wait()

    def x_step(grp):
        slot = lax.rem(grp, 2)
        for copy in load(grp, slot):
            copy.wait()

        def body(yy, peak):
            pieces = []
            for dy in range(2):
                y = yy * 2 + dy
                halves = [stage[slot, c, :, pl.ds(y, 1)].reshape(FG * B, N) for c in range(2)]
                pieces.append(jnp.concatenate(halves, axis=1))
            data = jnp.concatenate(pieces, axis=0)
            out = lax.dot_general(fx_ref[...], data, (((1,), (1,)), ((), ())), precision=highest,
                                  preferred_element_type=jnp.float32)
            for dy in range(2):
                for blk in range(2 * NP * NJ):
                    base = blk // 2 * MSG + blk % 2 * B + yy * 2 + dy
                    xout[pl.ds(base, KC, stride=2 * B), :] = out[blk * KC:(blk + 1) * KC, dy * N:(dy + 1) * N]
            tall = jnp.max(jnp.abs(out).reshape(2 * N // 8, 8, 2 * N), axis=0)
            return jnp.maximum(peak, jnp.maximum(tall[:, :N], tall[:, N:]))

        peak = lax.fori_loop(0, B // 2, body, jnp.zeros((8, N), jnp.float32))
        scale = scale_of(jnp.max(peak, axis=0, keepdims=True))
        tail = jnp.broadcast_to(scale, (SC, N)).astype(jnp.bfloat16)

        def send(j, _):
            t = grp * NJ + j
            place = lax.rem(t, 2 * NJ)

            def pack(r, _):
                rows = pl.ds(pl.multiple_of((r * NJ + j) * MSG, MSG), MSG)
                xsend[place, r, :MSG, :] = encode(xout[rows, :], scale)
                xsend[place, r, MSG:, :] = tail
                return 0

            lax.fori_loop(0, NP, pack, 0)
            for d in (2, 3, 1, 0):
                row_copy(t, d).start()
            return 0

        lax.fori_loop(0, NJ, send, 0)

    def row_drained(grp):
        def body(j, _):
            for d in (1, 2, 3):
                row_copy(grp * NJ + j, d).wait_send()
            return 0

        lax.fori_loop(0, NJ, body, 0)

    def y_step(t):
        slot = lax.rem(t, YS)
        arrived(xrecv, xr_sem, t)

        def body(kk, _):
            cols = []
            for dk in range(2):
                k = kk * 2 + dk
                rows = pl.ds(pl.multiple_of(k * 2 * B, 2 * B), 2 * B)
                cols.append(jnp.concatenate(
                    [decode(xrecv[t, p, rows, :], xrecv[t, p, MSG:, :].astype(jnp.float32)[:1]) for p in range(NP)],
                    axis=0))
            data = jnp.concatenate(cols, axis=1)
            out = jnp.dot(fy_ref[...], data, precision=highest, preferred_element_type=jnp.float32)
            scale = scale_of(jnp.max(jnp.abs(out), axis=0, keepdims=True))
            out = encode(out, scale)
            for dk in range(2):
                scales[pl.ds(kk * 2 + dk, 1), :] = scale[:, dk * N:(dk + 1) * N]
                for s in range(NP):
                    for c in range(2):
                        rows = pl.ds(pl.multiple_of(c * KC * B + (kk * 2 + dk) * B, B), B)
                        ysend[slot, s, rows, :] = out[(s * 2 + c) * B:(s * 2 + c + 1) * B, dk * N:(dk + 1) * N]
            return 0

        lax.fori_loop(0, KC // 2, body, 0)
        tail = jnp.concatenate([scales[...]] * (SC // KC), axis=0).astype(jnp.bfloat16)
        for s in range(NP):
            ysend[slot, s, MSG:MSG + SC, :] = tail
        for d in (2, 3, 1, 0):
            col_copy(t, d).start()

    def z_step(t):
        grp, j = t // NJ, lax.rem(t, NJ)
        arrived(yrecv, yr_sem, t)
        half = KC * B
        gain = g_ref[pl.ds(j * KC, KC)].reshape(half, N)
        group = lax.broadcasted_iota(jnp.int32, (MSG + SC, N), 1) // B
        for f in range(FG):
            code = None
            for q in range(NP):
                piece = yrecv[t, q]
                if q != f:
                    piece = pltpu.roll(piece, (q - f) % NP * B, 1)
                code = piece if code is None else jnp.where(group == q, piece, code)
            rows = code[MSG:].astype(jnp.float32)
            scale = jnp.concatenate([jnp.broadcast_to(rows[k:k + 1], (B, N)) for k in range(KC)], axis=0)
            data = jnp.concatenate([decode(code[c * half:(c + 1) * half], scale) for c in range(2)], axis=1)
            out = jnp.dot(data, fz_ref[...], precision=highest, preferred_element_type=jnp.float32)
            for c, dst in enumerate((wr_ref, wi_ref)):
                dst[grp * FG + f, pl.ds(j * KC, KC)] = (out[:, c * N:(c + 1) * N] * gain).reshape(KC, B, N)

    for grp in range(min(2, ng)):
        for copy in load(grp, grp):
            copy.start()

    barrier = pltpu.get_barrier_semaphore()
    for d in range(1, NP):
        pl.semaphore_signal(barrier, inc=1, device_id={"row": peer(row, d)}, device_id_type=MESH)
        pl.semaphore_signal(barrier, inc=1, device_id={"col": peer(col, d)}, device_id_type=MESH)
    pl.semaphore_wait(barrier, 2 * (NP - 1))

    x_step(0)

    if ng > 1:
        x_step(1)
    if ng > 2:
        for copy in load(2, 0):
            copy.start()

    def tick(t, _):
        @pl.when(t >= YS)
        def _():
            for d in (1, 2, 3):
                col_copy(t - YS, d).wait_send()

        y_step(t)

        @pl.when(t >= LAG)
        def _():
            z_step(t - LAG)

        if ng > 2:
            @pl.when((lax.rem(t, NJ) == NJ - 1) & (t < (ng - 2) * NJ))
            def _():
                grp = t // NJ
                row_drained(grp)
                x_step(grp + 2)

                @pl.when(grp + 3 < ng)
                def _():
                    for copy in load(grp + 3, lax.rem(grp + 3, 2)):
                        copy.start()

        return 0

    lax.fori_loop(0, nt, tick, 0)

    def drain(t, _):
        z_step(t)
        return 0

    lax.fori_loop(max(nt - LAG, 0), nt, drain, 0)
    for grp in range(max(ng - 2, 0), ng):
        row_drained(grp)
    for t in range(max(nt - YS, 0), nt):
        for d in (1, 2, 3):
            col_copy(t, d).wait_send()


def solution(mesh):
    fx, fy, fz = dft_tables()

    def local_forward(u_real, u_imag, g_filter):
        ng = u_real.shape[0] // FG
        nt = ng * NJ
        u_real, u_imag = (jnp.transpose(u, (0, 2, 3, 1)) for u in (u_real, u_imag))
        out = pltpu.VMEM((ng * FG, B, B, N), jnp.float32)
        vmem, anywhere = pl.BlockSpec(memory_space=pltpu.VMEM), pl.BlockSpec(memory_space=pl.ANY)
        flops = 2 * 2 * N * 2 * N * N * B * B // N * ng * FG * 24
        return pl.pallas_call(
            functools.partial(kernel, ng),
            out_shape=(out, out),
            in_specs=[vmem] * 4 + [anywhere] * 2,
            out_specs=(vmem, vmem),
            scratch_shapes=[
                pltpu.VMEM((2, 2, FG, B, B, N), jnp.float32),
                pltpu.VMEM((NP * NJ * MSG, N), jnp.float32),
                pltpu.VMEM((2 * NJ, NP, MSG + SC, N), jnp.bfloat16),
                pltpu.VMEM((nt, NP, MSG + SC, N), jnp.bfloat16),
                pltpu.VMEM((YS, NP, MSG + SC, N), jnp.bfloat16),
                pltpu.VMEM((nt, NP, MSG + SC, N), jnp.bfloat16),
                pltpu.VMEM((KC, N), jnp.float32),
                pltpu.SemaphoreType.DMA((2, 2)),
                pltpu.SemaphoreType.DMA((2 * NJ, NP)),
                pltpu.SemaphoreType.DMA((nt, NP)),
                pltpu.SemaphoreType.DMA((YS, NP)),
                pltpu.SemaphoreType.DMA((nt, NP)),
            ],
            compiler_params=pltpu.CompilerParams(
                collective_id=0, has_side_effects=True, vmem_limit_bytes=44 << 20),
            cost_estimate=pl.CostEstimate(flops=flops, bytes_accessed=1 << 25, transcendentals=0),
        )(jnp.asarray(fx), jnp.asarray(fy), jnp.asarray(fz), g_filter, u_real, u_imag)

    field_spec = P("fld", None, "row", "col")
    out_spec = P("fld", "row", "col", None)
    return jax.shard_map(local_forward, mesh=mesh, in_specs=(field_spec, field_spec, P("row", "col", None)),
                         out_specs=(out_spec, out_spec), check_vma=False)
```

```python
import functools
import math

import jax
import jax.numpy as jnp
import numpy as np
from jax import lax
from jax.experimental import pallas as pl
from jax.experimental.pallas import tpu as pltpu
from jax.sharding import PartitionSpec as P

MESH = pl.DeviceIdType.MESH
N = 128
B = 32
NP = 4
FG = 4
KC = 8
NJ = B // KC
MSG = 2 * KC * B
SC = 16
TINY = 2.0 ** -126
LAG = 6
YS = LAG + 2


def dft_tables():
    idx = np.arange(N)
    ang = 2.0 * np.pi * ((idx[:, None] * idx[None, :]) % N) / N
    cos, sin = np.cos(ang) / math.sqrt(N), np.sin(ang) / math.sqrt(N)
    mat = np.stack([np.stack([cos, sin], 1), np.stack([-sin, cos], 1)])
    fx = mat.reshape(2, NP, NJ, KC, 2 * N).transpose(2, 1, 0, 3, 4).reshape(2 * N, 2 * N)
    fy = mat.reshape(2, NP, B, 2, NP, B).transpose(1, 0, 2, 4, 3, 5).reshape(2 * N, 2 * N)
    fz = mat.transpose(2, 3, 0, 1).reshape(2 * N, 2 * N)
    return fx.astype(np.float32), fy.astype(np.float32), fz.astype(np.float32)


def encode(x, scale):
    v = x * (1.0 / scale)
    p = v * v
    p = p * p
    p = p * p
    return jnp.where(v < 0, -p, p).astype(jnp.bfloat16)


def decode(code, scale):
    y = code.astype(jnp.float32)
    p = jnp.maximum(jnp.abs(y), TINY)
    root = lax.rsqrt(lax.rsqrt(p * lax.rsqrt(p)))
    return jnp.where(y == 0, 0.0, jnp.where(y < 0, -root, root)) * scale


def scale_of(x):
    return jnp.maximum(x, TINY).astype(jnp.bfloat16).astype(jnp.float32)


def kernel(ng, fx_ref, fy_ref, fz_ref, g_ref, ur_ref, ui_ref, wr_ref, wi_ref,
           stage, xout, xsend, xrecv, ysend, yrecv, ssend, srecv,
           in_sem, xs_sem, xr_sem, ys_sem, yr_sem, ss_sem, sr_sem):
    nt = ng * NJ
    col, row = lax.axis_index("col"), lax.axis_index("row")
    highest = lax.Precision.HIGHEST

    def peer(me, d):
        return (me, me + 1 - 2 * lax.rem(me, 2), lax.rem(me + 2, NP), NP - 1 - me)[d]

    def load(grp, slot):
        copies = []
        for c, src in enumerate((ur_ref, ui_ref)):
            copies.append(pltpu.make_async_copy(src.at[pl.ds(grp * FG, FG)], stage.at[slot, c], in_sem.at[slot, c]))
        return copies

    def row_copy(t, d):
        dst = peer(row, d)
        src = xsend.at[lax.rem(t, 2 * NJ), dst]
        if d == 0:
            return pltpu.make_async_copy(src, xrecv.at[t, row], xr_sem.at[t, row])
        return pltpu.make_async_remote_copy(
            src, xrecv.at[t, row], xs_sem.at[lax.rem(t, 2 * NJ), d], xr_sem.at[t, row],
            device_id={"row": dst}, device_id_type=MESH)

    def col_copy(t, d):
        dst = peer(col, d)
        src = ysend.at[lax.rem(t, YS), dst]
        if d == 0:
            return pltpu.make_async_copy(src, yrecv.at[t, col], yr_sem.at[t, col])
        return pltpu.make_async_remote_copy(
            src, yrecv.at[t, col], ys_sem.at[lax.rem(t, YS), d], yr_sem.at[t, col],
            device_id={"col": dst}, device_id_type=MESH)

    def scale_copy(grp, d):
        dst = peer(col, d)
        src = ssend.at[grp]
        if d == 0:
            return pltpu.make_async_copy(src, srecv.at[grp, col], sr_sem.at[grp, col])
        return pltpu.make_async_remote_copy(
            src, srecv.at[grp, col], ss_sem.at[grp, d], sr_sem.at[grp, col],
            device_id={"col": dst}, device_id_type=MESH)

    def arrived(buf, sem, t):
        for p in range(NP):
            pltpu.make_async_copy(buf.at[t, p], buf.at[t, p], sem.at[t, p]).wait()

    def row_scale(grp):
        slot = lax.rem(grp, 2)
        for copy in load(grp, slot):
            copy.wait()

        def body(y, peaks):
            blocks = [jnp.abs(stage[slot, :, f, pl.ds(y, 1)]).reshape(2 * B // 8, 8, N) for f in range(FG)]
            return tuple(jnp.maximum(peak, jnp.max(block, axis=0)) for peak, block in zip(peaks, blocks))

        peaks = lax.fori_loop(0, B, body, (jnp.zeros((8, N), jnp.float32),) * FG)
        field = lax.broadcasted_iota(jnp.int32, (1, N), 1) // B
        scale = jnp.zeros((1, N), jnp.float32)
        for f, peak in enumerate(peaks):
            peak = jnp.max(jnp.max(peak, axis=1, keepdims=True), axis=0, keepdims=True)
            scale = jnp.where(field == f, peak, scale)
        return scale_of(scale * 2.0 ** -11)

    def x_step(grp, scale, lo, hi):
        slot = lax.rem(grp, 2)

        def body(yy, _):
            pieces = []
            for dy in range(2):
                y = yy * 2 + dy
                halves = [stage[slot, c, :, pl.ds(y, 1)].reshape(FG * B, N) for c in range(2)]
                pieces.append(jnp.concatenate(halves, axis=1))
            data = jnp.concatenate(pieces, axis=0)
            rows = 2 * NP * KC
            out = lax.dot_general(fx_ref[lo * rows:hi * rows, :], data, (((1,), (1,)), ((), ())), precision=highest,
                                  preferred_element_type=jnp.float32)
            for dy in range(2):
                for blk in range((hi - lo) * NP * 2):
                    base = (lo * NP + blk // 2) * MSG + blk % 2 * B + yy * 2 + dy
                    xout[pl.ds(base, KC, stride=2 * B), :] = out[blk * KC:(blk + 1) * KC, dy * N:(dy + 1) * N]
            return 0

        lax.fori_loop(0, B // 2, body, 0)
        tail = jnp.broadcast_to(scale, (SC, N)).astype(jnp.bfloat16)

        def send(j, _):
            t = grp * NJ + j
            place = lax.rem(t, 2 * NJ)

            def pack(r, _):
                rows = pl.ds(pl.multiple_of((j * NP + r) * MSG, MSG), MSG)
                xsend[place, r, :MSG, :] = encode(xout[rows, :], scale)
                xsend[place, r, MSG:, :] = tail
                return 0

            lax.fori_loop(0, NP, pack, 0)
            for d in (2, 3, 1, 0):
                row_copy(t, d).start()
            return 0

        lax.fori_loop(lo, hi, send, 0)

    def row_drained(grp):
        def body(j, _):
            for d in (1, 2, 3):
                row_copy(grp * NJ + j, d).wait_send()
            return 0

        lax.fori_loop(0, NJ, body, 0)

    def y_step(t):
        slot = lax.rem(t, YS)
        arrived(xrecv, xr_sem, t)
        given = [xrecv[t, p, MSG:, :].astype(jnp.float32)[:1] for p in range(NP)]
        scale = scale_of(4.0 * sum(given))

        @pl.when(lax.rem(t, NJ) == 0)
        def _():
            ssend[t // NJ] = jnp.broadcast_to(scale, (SC, N)).astype(jnp.bfloat16)
            for d in (2, 3, 1, 0):
                scale_copy(t // NJ, d).start()

        scale2 = jnp.concatenate([scale, scale], axis=1)

        def body(kk, _):
            cols = []
            for dk in range(2):
                k = kk * 2 + dk
                rows = pl.ds(pl.multiple_of(k * 2 * B, 2 * B), 2 * B)
                cols.append(jnp.concatenate(
                    [decode(xrecv[t, p, rows, :], given[p]) for p in range(NP)],
                    axis=0))
            data = jnp.concatenate(cols, axis=1)
            out = jnp.dot(fy_ref[...], data, precision=highest, preferred_element_type=jnp.float32)
            out = encode(out, scale2)
            for dk in range(2):
                for s in range(NP):
                    for c in range(2):
                        rows = pl.ds(pl.multiple_of(c * KC * B + (kk * 2 + dk) * B, B), B)
                        ysend[slot, s, rows, :] = out[(s * 2 + c) * B:(s * 2 + c + 1) * B, dk * N:(dk + 1) * N]
            return 0

        lax.fori_loop(0, KC // 2, body, 0)
        for d in (2, 3, 1, 0):
            col_copy(t, d).start()

    def z_step(t):
        grp, j = t // NJ, lax.rem(t, NJ)
        @pl.when(j == 0)
        def _():
            arrived(srecv, sr_sem, grp)

        arrived(yrecv, yr_sem, t)
        half = KC * B
        gain = g_ref[pl.ds(j * KC, KC)].reshape(half, N)
        def take(f, pieces):
            group = lax.broadcasted_iota(jnp.int32, pieces[0].shape, 1) // B
            code = None
            for q, piece in enumerate(pieces):
                if q != f:
                    piece = pltpu.roll(piece, (q - f) % NP * B, 1)
                code = piece if code is None else jnp.where(group == q, piece, code)
            return code

        for f in range(FG):
            code = take(f, [yrecv[t, q] for q in range(NP)])
            scale = take(f, [srecv[grp, q].astype(jnp.float32) for q in range(NP)])[:1]
            data = jnp.concatenate([decode(code[c * half:(c + 1) * half], scale) for c in range(2)], axis=1)
            out = jnp.dot(data, fz_ref[...], precision=highest, preferred_element_type=jnp.float32)
            for c, dst in enumerate((wr_ref, wi_ref)):
                dst[grp * FG + f, pl.ds(j * KC, KC)] = (out[:, c * N:(c + 1) * N] * gain).reshape(KC, B, N)

    for grp in range(min(2, ng)):
        for copy in load(grp, grp):
            copy.start()

    barrier = pltpu.get_barrier_semaphore()
    for d in range(1, NP):
        pl.semaphore_signal(barrier, inc=1, device_id={"row": peer(row, d)}, device_id_type=MESH)
        pl.semaphore_signal(barrier, inc=1, device_id={"col": peer(col, d)}, device_id_type=MESH)
    pl.semaphore_wait(barrier, 2 * (NP - 1))

    scale0 = row_scale(0)
    x_step(0, scale0, 0, 1)
    x_step(0, scale0, 1, NJ)
    if ng > 2:
        for copy in load(2, 0):
            copy.start()

    def tick(t, _):
        @pl.when(t >= YS)
        def _():
            for d in (1, 2, 3):
                col_copy(t - YS, d).wait_send()

        y_step(t)

        if ng > 1:
            @pl.when(t == 0)
            def _():
                x_step(1, row_scale(1), 0, NJ)

        @pl.when(t >= LAG)
        def _():
            z_step(t - LAG)

        if ng > 2:
            @pl.when((lax.rem(t, NJ) == NJ - 1) & (t < (ng - 2) * NJ))
            def _():
                grp = t // NJ
                row_drained(grp)
                x_step(grp + 2, row_scale(grp + 2), 0, NJ)

                @pl.when(grp + 3 < ng)
                def _():
                    for copy in load(grp + 3, lax.rem(grp + 3, 2)):
                        copy.start()

        return 0

    lax.fori_loop(0, nt, tick, 0)

    def drain(t, _):
        z_step(t)
        return 0

    lax.fori_loop(max(nt - LAG, 0), nt, drain, 0)
    for grp in range(max(ng - 2, 0), ng):
        row_drained(grp)
    for t in range(max(nt - YS, 0), nt):
        for d in (1, 2, 3):
            col_copy(t, d).wait_send()
    for grp in range(ng):
        for d in (1, 2, 3):
            scale_copy(grp, d).wait_send()


def solution(mesh):
    fx, fy, fz = dft_tables()

    def local_forward(u_real, u_imag, g_filter):
        ng = u_real.shape[0] // FG
        nt = ng * NJ
        u_real, u_imag = (jnp.transpose(u, (0, 2, 3, 1)) for u in (u_real, u_imag))
        out = pltpu.VMEM((ng * FG, B, B, N), jnp.float32)
        vmem, anywhere = pl.BlockSpec(memory_space=pltpu.VMEM), pl.BlockSpec(memory_space=pl.ANY)
        flops = 2 * 2 * N * 2 * N * N * B * B // N * ng * FG * 24
        return pl.pallas_call(
            functools.partial(kernel, ng),
            out_shape=(out, out),
            in_specs=[vmem] * 4 + [anywhere] * 2,
            out_specs=(vmem, vmem),
            scratch_shapes=[
                pltpu.VMEM((2, 2, FG, B, B, N), jnp.float32),
                pltpu.VMEM((NP * NJ * MSG, N), jnp.float32),
                pltpu.VMEM((2 * NJ, NP, MSG + SC, N), jnp.bfloat16),
                pltpu.VMEM((nt, NP, MSG + SC, N), jnp.bfloat16),
                pltpu.VMEM((YS, NP, MSG, N), jnp.bfloat16),
                pltpu.VMEM((nt, NP, MSG, N), jnp.bfloat16),
                pltpu.VMEM((ng, SC, N), jnp.bfloat16),
                pltpu.VMEM((ng, NP, SC, N), jnp.bfloat16),
                pltpu.SemaphoreType.DMA((2, 2)),
                pltpu.SemaphoreType.DMA((2 * NJ, NP)),
                pltpu.SemaphoreType.DMA((nt, NP)),
                pltpu.SemaphoreType.DMA((YS, NP)),
                pltpu.SemaphoreType.DMA((nt, NP)),
                pltpu.SemaphoreType.DMA((ng, NP)),
                pltpu.SemaphoreType.DMA((ng, NP)),
            ],
            compiler_params=pltpu.CompilerParams(
                collective_id=0, has_side_effects=True, vmem_limit_bytes=44 << 20),
            cost_estimate=pl.CostEstimate(flops=flops, bytes_accessed=1 << 25, transcendentals=0),
        )(jnp.asarray(fx), jnp.asarray(fy), jnp.asarray(fz), g_filter, u_real, u_imag)

    field_spec = P("fld", None, "row", "col")
    out_spec = P("fld", "row", "col", None)
    return jax.shard_map(local_forward, mesh=mesh, in_specs=(field_spec, field_spec, P("row", "col", None)),
                         out_specs=(out_spec, out_spec), check_vma=False)
```

```python
import functools
import math

import jax
import jax.numpy as jnp
import numpy as np
from jax import lax
from jax.experimental import pallas as pl
from jax.experimental.pallas import tpu as pltpu
from jax.sharding import PartitionSpec as P

MESH = pl.DeviceIdType.MESH
N = 128
B = 32
NP = 4
FG = 4
KC = 8
NJ = B // KC
MSG = 2 * KC * B
SC = 16
TINY = 2.0 ** -126
LAG = 6
YS = LAG + 2


def dft_tables():
    idx = np.arange(N)
    ang = 2.0 * np.pi * ((idx[:, None] * idx[None, :]) % N) / N
    cos, sin = np.cos(ang) / math.sqrt(N), np.sin(ang) / math.sqrt(N)
    mat = np.stack([np.stack([cos, sin], 1), np.stack([-sin, cos], 1)])
    fx = mat.reshape(2, NP, NJ, KC, 2 * N).transpose(2, 1, 0, 3, 4).reshape(2 * N, 2 * N)
    fy = mat.reshape(2, NP, B, 2, NP, B).transpose(1, 0, 2, 4, 3, 5).reshape(2 * N, 2 * N)
    fz = mat.transpose(2, 3, 0, 1).reshape(2 * N, 2 * N)
    return fx.astype(np.float32), fy.astype(np.float32), fz.astype(np.float32)


def encode(x, scale):
    v = x * (1.0 / scale)
    p = v * v
    p = p * p
    p = p * p
    return jnp.where(v < 0, -p, p).astype(jnp.bfloat16)


def decode(code, scale):
    y = code.astype(jnp.float32)
    p = jnp.maximum(jnp.abs(y), TINY)
    root = lax.rsqrt(lax.rsqrt(p * lax.rsqrt(p)))
    return jnp.where(y == 0, 0.0, jnp.where(y < 0, -root, root)) * scale


def scale_of(x):
    return jnp.maximum(x, TINY).astype(jnp.bfloat16).astype(jnp.float32)


def take(f, pieces):
    group = lax.broadcasted_iota(jnp.int32, pieces[0].shape, 1) // B
    code = None
    for q, piece in enumerate(pieces):
        if q != f:
            piece = pltpu.roll(piece, (q - f) % NP * B, 1)
        code = piece if code is None else jnp.where(group == q, piece, code)
    return code


def z_field(f, codes, scales, fz_ref, gain):
    half = KC * B
    code = take(f, codes)
    scale = take(f, [s.astype(jnp.float32) for s in scales])[:1]
    data = jnp.concatenate([decode(code[c * half:(c + 1) * half], scale) for c in range(2)], axis=1)
    out = jnp.dot(data, fz_ref[...], precision=lax.Precision.HIGHEST, preferred_element_type=jnp.float32)
    return [(out[:, c * N:(c + 1) * N] * gain).reshape(KC, B, N) for c in range(2)]


def finish(ng, fz_ref, g_ref, wr_ref, wi_ref, code_ref, scale_ref, or_ref, oi_ref, stage, sem, last_sem):
    kx, done = (NJ - 1) * KC, (ng - 1) * FG
    copies = []
    for c, (src, dst) in enumerate(((wr_ref, or_ref), (wi_ref, oi_ref))):
        tail = (pl.ds(done, FG), pl.ds(0, kx))
        copies.append(pltpu.make_async_copy(src.at[tail], dst.at[tail], sem.at[c, 0]))
        if done:
            copies.append(pltpu.make_async_copy(src.at[pl.ds(0, done)], dst.at[pl.ds(0, done)], sem.at[c, 1]))
    for copy in copies:
        copy.start()
    gain = g_ref[kx:].reshape(KC * B, N)
    for f in range(FG):
        parts = z_field(f, [code_ref[q] for q in range(NP)], [scale_ref[q] for q in range(NP)], fz_ref, gain)
        for c, (part, dst) in enumerate(zip(parts, (or_ref, oi_ref))):
            stage[c, f] = part
            copy = pltpu.make_async_copy(stage.at[c, f], dst.at[done + f, pl.ds(kx, KC)], last_sem.at[c, f])
            copy.start()
            copies.append(copy)
    for copy in copies:
        copy.wait()


def kernel(ng, fx_ref, fy_ref, fz_ref, g_ref, ur_ref, ui_ref, wr_ref, wi_ref, code_ref, scale_ref,
           stage, xout, xsend, xrecv, ysend, yrecv, ssend, srecv,
           in_sem, xs_sem, xr_sem, ys_sem, yr_sem, ss_sem, sr_sem):
    nt = ng * NJ
    col, row = lax.axis_index("col"), lax.axis_index("row")
    highest = lax.Precision.HIGHEST

    def peer(me, d):
        return (me, me + 1 - 2 * lax.rem(me, 2), lax.rem(me + 2, NP), NP - 1 - me)[d]

    def load(grp, slot):
        copies = []
        for c, src in enumerate((ur_ref, ui_ref)):
            copies.append(pltpu.make_async_copy(src.at[pl.ds(grp * FG, FG)], stage.at[slot, c], in_sem.at[slot, c]))
        return copies

    def row_copy(t, d):
        dst = peer(row, d)
        src = xsend.at[lax.rem(t, 2 * NJ), dst]
        if d == 0:
            return pltpu.make_async_copy(src, xrecv.at[t, row], xr_sem.at[t, row])
        return pltpu.make_async_remote_copy(
            src, xrecv.at[t, row], xs_sem.at[lax.rem(t, 2 * NJ), d], xr_sem.at[t, row],
            device_id={"row": dst}, device_id_type=MESH)

    def col_copy(t, d):
        dst = peer(col, d)
        src = ysend.at[lax.rem(t, YS), dst]
        if d == 0:
            return pltpu.make_async_copy(src, yrecv.at[t, col], yr_sem.at[t, col])
        return pltpu.make_async_remote_copy(
            src, yrecv.at[t, col], ys_sem.at[lax.rem(t, YS), d], yr_sem.at[t, col],
            device_id={"col": dst}, device_id_type=MESH)

    def scale_copy(grp, d):
        dst = peer(col, d)
        src = ssend.at[grp]
        if d == 0:
            return pltpu.make_async_copy(src, srecv.at[grp, col], sr_sem.at[grp, col])
        return pltpu.make_async_remote_copy(
            src, srecv.at[grp, col], ss_sem.at[grp, d], sr_sem.at[grp, col],
            device_id={"col": dst}, device_id_type=MESH)

    def arrived(buf, sem, t):
        for p in range(NP):
            pltpu.make_async_copy(buf.at[t, p], buf.at[t, p], sem.at[t, p]).wait()

    def row_scale(grp):
        slot = lax.rem(grp, 2)
        for copy in load(grp, slot):
            copy.wait()

        def body(y, peaks):
            blocks = [jnp.abs(stage[slot, :, f, pl.ds(y, 1)]).reshape(2 * B // 8, 8, N) for f in range(FG)]
            return tuple(jnp.maximum(peak, jnp.max(block, axis=0)) for peak, block in zip(peaks, blocks))

        peaks = lax.fori_loop(0, B, body, (jnp.zeros((8, N), jnp.float32),) * FG)
        field = lax.broadcasted_iota(jnp.int32, (1, N), 1) // B
        scale = jnp.zeros((1, N), jnp.float32)
        for f, peak in enumerate(peaks):
            peak = jnp.max(jnp.max(peak, axis=1, keepdims=True), axis=0, keepdims=True)
            scale = jnp.where(field == f, peak, scale)
        return scale_of(scale * 2.0 ** -11)

    def x_step(grp, scale, lo, hi):
        slot = lax.rem(grp, 2)

        def body(yy, _):
            pieces = []
            for dy in range(2):
                y = yy * 2 + dy
                halves = [stage[slot, c, :, pl.ds(y, 1)].reshape(FG * B, N) for c in range(2)]
                pieces.append(jnp.concatenate(halves, axis=1))
            data = jnp.concatenate(pieces, axis=0)
            rows = 2 * NP * KC
            out = lax.dot_general(fx_ref[lo * rows:hi * rows, :], data, (((1,), (1,)), ((), ())), precision=highest,
                                  preferred_element_type=jnp.float32)
            for dy in range(2):
                for blk in range((hi - lo) * NP * 2):
                    base = (lo * NP + blk // 2) * MSG + blk % 2 * B + yy * 2 + dy
                    xout[pl.ds(base, KC, stride=2 * B), :] = out[blk * KC:(blk + 1) * KC, dy * N:(dy + 1) * N]
            return 0

        lax.fori_loop(0, B // 2, body, 0)
        tail = jnp.broadcast_to(scale, (SC, N)).astype(jnp.bfloat16)

        def send(j, _):
            t = grp * NJ + j
            place = lax.rem(t, 2 * NJ)

            def pack(r, _):
                rows = pl.ds(pl.multiple_of((j * NP + r) * MSG, MSG), MSG)
                xsend[place, r, :MSG, :] = encode(xout[rows, :], scale)
                xsend[place, r, MSG:, :] = tail
                return 0

            lax.fori_loop(0, NP, pack, 0)
            for d in (2, 3, 1, 0):
                row_copy(t, d).start()
            return 0

        lax.fori_loop(lo, hi, send, 0)

    def row_drained(grp):
        def body(j, _):
            for d in (1, 2, 3):
                row_copy(grp * NJ + j, d).wait_send()
            return 0

        lax.fori_loop(0, NJ, body, 0)

    def y_step(t):
        slot = lax.rem(t, YS)
        arrived(xrecv, xr_sem, t)
        given = [xrecv[t, p, MSG:, :].astype(jnp.float32)[:1] for p in range(NP)]
        scale = scale_of(4.0 * sum(given))

        @pl.when(lax.rem(t, NJ) == 0)
        def _():
            ssend[t // NJ] = jnp.broadcast_to(scale, (SC, N)).astype(jnp.bfloat16)
            for d in (2, 3, 1, 0):
                scale_copy(t // NJ, d).start()

        scale2 = jnp.concatenate([scale, scale], axis=1)

        def body(kk, _):
            cols = []
            for dk in range(2):
                k = kk * 2 + dk
                rows = pl.ds(pl.multiple_of(k * 2 * B, 2 * B), 2 * B)
                cols.append(jnp.concatenate(
                    [decode(xrecv[t, p, rows, :], given[p]) for p in range(NP)],
                    axis=0))
            data = jnp.concatenate(cols, axis=1)
            out = jnp.dot(fy_ref[...], data, precision=highest, preferred_element_type=jnp.float32)
            out = encode(out, scale2)
            for dk in range(2):
                for s in range(NP):
                    for c in range(2):
                        rows = pl.ds(pl.multiple_of(c * KC * B + (kk * 2 + dk) * B, B), B)
                        ysend[slot, s, rows, :] = out[(s * 2 + c) * B:(s * 2 + c + 1) * B, dk * N:(dk + 1) * N]
            return 0

        lax.fori_loop(0, KC // 2, body, 0)
        @pl.when(t < nt - 1)
        def _():
            for d in (2, 3, 1, 0):
                col_copy(t, d).start()

        @pl.when(t == nt - 1)
        def _():
            for d in (1, 2, 3, 0):
                col_copy(t, d).start()


    def z_step(t):
        grp, j = t // NJ, lax.rem(t, NJ)
        @pl.when(j == 0)
        def _():
            arrived(srecv, sr_sem, grp)

        arrived(yrecv, yr_sem, t)
        gain = g_ref[pl.ds(j * KC, KC)].reshape(KC * B, N)
        for f in range(FG):
            parts = z_field(f, [yrecv[t, q] for q in range(NP)], [srecv[grp, q] for q in range(NP)], fz_ref, gain)
            for part, dst in zip(parts, (wr_ref, wi_ref)):
                dst[grp * FG + f, pl.ds(j * KC, KC)] = part

    for grp in range(min(2, ng)):
        for copy in load(grp, grp):
            copy.start()

    barrier = pltpu.get_barrier_semaphore()
    for d in range(1, NP):
        pl.semaphore_signal(barrier, inc=1, device_id={"row": peer(row, d)}, device_id_type=MESH)
        pl.semaphore_signal(barrier, inc=1, device_id={"col": peer(col, d)}, device_id_type=MESH)
    pl.semaphore_wait(barrier, 2 * (NP - 1))

    scale0 = row_scale(0)
    x_step(0, scale0, 0, 1)
    x_step(0, scale0, 1, NJ)
    if ng > 2:
        for copy in load(2, 0):
            copy.start()

    def tick(t, _):
        @pl.when(t >= YS)
        def _():
            for d in (1, 2, 3):
                col_copy(t - YS, d).wait_send()

        y_step(t)

        if ng > 1:
            @pl.when(t == 1)
            def _():
                x_step(1, row_scale(1), 0, NJ)

        @pl.when(t >= LAG)
        def _():
            z_step(t - LAG)

        if ng > 2:
            @pl.when((lax.rem(t, NJ) == NJ - 1) & (t < (ng - 2) * NJ))
            def _():
                grp = t // NJ
                row_drained(grp)
                x_step(grp + 2, row_scale(grp + 2), 0, NJ)

                @pl.when(grp + 3 < ng)
                def _():
                    for copy in load(grp + 3, lax.rem(grp + 3, 2)):
                        copy.start()

        return 0

    lax.fori_loop(0, nt, tick, 0)

    def drain(t, _):
        z_step(t)
        return 0

    lax.fori_loop(max(nt - LAG, 0), nt - 1, drain, 0)
    arrived(yrecv, yr_sem, nt - 1)
    for q in range(NP):
        code_ref[q] = yrecv[nt - 1, q]
        scale_ref[q] = srecv[ng - 1, q]
    for grp in range(max(ng - 2, 0), ng):
        row_drained(grp)
    for t in range(max(nt - YS, 0), nt):
        for d in (1, 2, 3):
            col_copy(t, d).wait_send()
    for grp in range(ng):
        for d in (1, 2, 3):
            scale_copy(grp, d).wait_send()


def solution(mesh):
    fx, fy, fz = dft_tables()

    def local_forward(u_real, u_imag, g_filter):
        ng = u_real.shape[0] // FG
        nt = ng * NJ
        u_real, u_imag = (jnp.transpose(u, (0, 2, 3, 1)) for u in (u_real, u_imag))
        out = pltpu.VMEM((ng * FG, B, B, N), jnp.float32)
        vmem, anywhere = pl.BlockSpec(memory_space=pltpu.VMEM), pl.BlockSpec(memory_space=pl.ANY)
        flops = 2 * 2 * N * 2 * N * N * B * B // N * ng * FG * 24
        w_real, w_imag, code, scale = pl.pallas_call(
            functools.partial(kernel, ng),
            out_shape=(out, out, pltpu.VMEM((NP, MSG, N), jnp.bfloat16), pltpu.VMEM((NP, SC, N), jnp.bfloat16)),
            in_specs=[vmem] * 4 + [anywhere] * 2,
            out_specs=(vmem,) * 4,
            scratch_shapes=[
                pltpu.VMEM((2, 2, FG, B, B, N), jnp.float32),
                pltpu.VMEM((NP * NJ * MSG, N), jnp.float32),
                pltpu.VMEM((2 * NJ, NP, MSG + SC, N), jnp.bfloat16),
                pltpu.VMEM((nt, NP, MSG + SC, N), jnp.bfloat16),
                pltpu.VMEM((YS, NP, MSG, N), jnp.bfloat16),
                pltpu.VMEM((nt, NP, MSG, N), jnp.bfloat16),
                pltpu.VMEM((ng, SC, N), jnp.bfloat16),
                pltpu.VMEM((ng, NP, SC, N), jnp.bfloat16),
                pltpu.SemaphoreType.DMA((2, 2)),
                pltpu.SemaphoreType.DMA((2 * NJ, NP)),
                pltpu.SemaphoreType.DMA((nt, NP)),
                pltpu.SemaphoreType.DMA((YS, NP)),
                pltpu.SemaphoreType.DMA((nt, NP)),
                pltpu.SemaphoreType.DMA((ng, NP)),
                pltpu.SemaphoreType.DMA((ng, NP)),
            ],
            compiler_params=pltpu.CompilerParams(
                collective_id=0, has_side_effects=True, vmem_limit_bytes=44 << 20),
            cost_estimate=pl.CostEstimate(flops=flops, bytes_accessed=1 << 25, transcendentals=0),
        )(jnp.asarray(fx), jnp.asarray(fy), jnp.asarray(fz), g_filter, u_real, u_imag)
        result = jax.ShapeDtypeStruct((ng * FG, B, B, N), jnp.float32)
        return pl.pallas_call(
            functools.partial(finish, ng),
            out_shape=(result, result),
            in_specs=[vmem] * 6,
            out_specs=(anywhere, anywhere),
            scratch_shapes=[
                pltpu.VMEM((2, FG, KC, B, N), jnp.float32),
                pltpu.SemaphoreType.DMA((2, 2)),
                pltpu.SemaphoreType.DMA((2, FG)),
            ],
            compiler_params=pltpu.CompilerParams(vmem_limit_bytes=16 << 20),
        )(jnp.asarray(fz), g_filter, w_real, w_imag, code, scale)

    field_spec = P("fld", None, "row", "col")
    out_spec = P("fld", "row", "col", None)
    return jax.shard_map(local_forward, mesh=mesh, in_specs=(field_spec, field_spec, P("row", "col", None)),
                         out_specs=(out_spec, out_spec), check_vma=False)
```

```python
import functools
import math

import jax
import jax.numpy as jnp
import numpy as np
from jax import lax
from jax.experimental import pallas as pl
from jax.experimental.pallas import tpu as pltpu
from jax.sharding import PartitionSpec as P

MESH = pl.DeviceIdType.MESH
N = 128
B = 32
NP = 4
FG = 4
KC = 4
NJ = B // KC
MSG = 2 * KC * B
SC = 16
TINY = 2.0 ** -126
LAG = 12
YS = LAG + 2


def dft_tables():
    idx = np.arange(N)
    ang = 2.0 * np.pi * ((idx[:, None] * idx[None, :]) % N) / N
    cos, sin = np.cos(ang) / math.sqrt(N), np.sin(ang) / math.sqrt(N)
    mat = np.stack([np.stack([cos, sin], 1), np.stack([-sin, cos], 1)])
    fx = mat.reshape(2, NP, NJ, KC, 2 * N).transpose(2, 1, 0, 3, 4).reshape(2 * N, 2 * N)
    fy = mat.reshape(2, NP, B, 2, NP, B).transpose(1, 0, 2, 4, 3, 5).reshape(2 * N, 2 * N)
    fz = mat.transpose(2, 3, 0, 1).reshape(2 * N, 2 * N)
    return fx.astype(np.float32), fy.astype(np.float32), fz.astype(np.float32)


def encode(x, scale):
    v = x * (1.0 / scale)
    p = v * v
    p = p * p
    p = p * p
    return jnp.where(v < 0, -p, p).astype(jnp.bfloat16)


def decode(code, scale):
    y = code.astype(jnp.float32)
    p = jnp.maximum(jnp.abs(y), TINY)
    root = lax.rsqrt(lax.rsqrt(p * lax.rsqrt(p)))
    return jnp.where(y == 0, 0.0, jnp.where(y < 0, -root, root)) * scale


def scale_of(x):
    return jnp.maximum(x, TINY).astype(jnp.bfloat16).astype(jnp.float32)


def take(f, pieces):
    group = lax.broadcasted_iota(jnp.int32, pieces[0].shape, 1) // B
    code = None
    for q, piece in enumerate(pieces):
        if q != f:
            piece = pltpu.roll(piece, (q - f) % NP * B, 1)
        code = piece if code is None else jnp.where(group == q, piece, code)
    return code


def z_field(f, codes, scales, fz_ref, gain):
    half = KC * B
    code = take(f, codes)
    scale = take(f, [s.astype(jnp.float32) for s in scales])[:1]
    data = jnp.concatenate([decode(code[c * half:(c + 1) * half], scale) for c in range(2)], axis=1)
    out = jnp.dot(data, fz_ref[...], precision=lax.Precision.HIGHEST, preferred_element_type=jnp.float32)
    return [(out[:, c * N:(c + 1) * N] * gain).reshape(KC, B, N) for c in range(2)]


def finish(ng, fz_ref, g_ref, wr_ref, wi_ref, code_ref, scale_ref, or_ref, oi_ref, stage, sem, last_sem):
    kx, done = (NJ - 1) * KC, (ng - 1) * FG
    copies = []
    for c, (src, dst) in enumerate(((wr_ref, or_ref), (wi_ref, oi_ref))):
        tail = (pl.ds(done, FG), pl.ds(0, kx))
        copies.append(pltpu.make_async_copy(src.at[tail], dst.at[tail], sem.at[c, 0]))
        if done:
            copies.append(pltpu.make_async_copy(src.at[pl.ds(0, done)], dst.at[pl.ds(0, done)], sem.at[c, 1]))
    for copy in copies:
        copy.start()
    gain = g_ref[kx:].reshape(KC * B, N)
    for f in range(FG):
        parts = z_field(f, [code_ref[q] for q in range(NP)], [scale_ref[q] for q in range(NP)], fz_ref, gain)
        for c, (part, dst) in enumerate(zip(parts, (or_ref, oi_ref))):
            stage[c, f] = part
            copy = pltpu.make_async_copy(stage.at[c, f], dst.at[done + f, pl.ds(kx, KC)], last_sem.at[c, f])
            copy.start()
            copies.append(copy)
    for copy in copies:
        copy.wait()


def kernel(ng, fx_ref, fy_ref, fz_ref, g_ref, ur_ref, ui_ref, wr_ref, wi_ref, code_ref, scale_ref,
           stage, xout, xsend, xrecv, ysend, yrecv, ssend, srecv,
           in_sem, xs_sem, xr_sem, ys_sem, yr_sem, ss_sem, sr_sem):
    nt = ng * NJ
    col, row = lax.axis_index("col"), lax.axis_index("row")
    highest = lax.Precision.HIGHEST

    def peer(me, d):
        return (me, me + 1 - 2 * lax.rem(me, 2), lax.rem(me + 2, NP), NP - 1 - me)[d]

    def load(grp, slot):
        copies = []
        for c, src in enumerate((ur_ref, ui_ref)):
            copies.append(pltpu.make_async_copy(src.at[pl.ds(grp * FG, FG)], stage.at[slot, c], in_sem.at[slot, c]))
        return copies

    def row_copy(t, d):
        dst = peer(row, d)
        src = xsend.at[lax.rem(t, 2 * NJ), dst]
        if d == 0:
            return pltpu.make_async_copy(src, xrecv.at[t, row], xr_sem.at[t, row])
        return pltpu.make_async_remote_copy(
            src, xrecv.at[t, row], xs_sem.at[lax.rem(t, 2 * NJ), d], xr_sem.at[t, row],
            device_id={"row": dst}, device_id_type=MESH)

    def col_copy(t, d):
        dst = peer(col, d)
        src = ysend.at[lax.rem(t, YS), dst]
        if d == 0:
            return pltpu.make_async_copy(src, yrecv.at[t, col], yr_sem.at[t, col])
        return pltpu.make_async_remote_copy(
            src, yrecv.at[t, col], ys_sem.at[lax.rem(t, YS), d], yr_sem.at[t, col],
            device_id={"col": dst}, device_id_type=MESH)

    def scale_copy(grp, d):
        dst = peer(col, d)
        src = ssend.at[grp]
        if d == 0:
            return pltpu.make_async_copy(src, srecv.at[grp, col], sr_sem.at[grp, col])
        return pltpu.make_async_remote_copy(
            src, srecv.at[grp, col], ss_sem.at[grp, d], sr_sem.at[grp, col],
            device_id={"col": dst}, device_id_type=MESH)

    def arrived(buf, sem, t):
        for p in range(NP):
            pltpu.make_async_copy(buf.at[t, p], buf.at[t, p], sem.at[t, p]).wait()

    def row_scale(grp):
        slot = lax.rem(grp, 2)
        for copy in load(grp, slot):
            copy.wait()

        def body(y, peaks):
            blocks = [jnp.abs(stage[slot, :, f, pl.ds(y, 1)]).reshape(2 * B // 8, 8, N) for f in range(FG)]
            return tuple(jnp.maximum(peak, jnp.max(block, axis=0)) for peak, block in zip(peaks, blocks))

        peaks = lax.fori_loop(0, B, body, (jnp.zeros((8, N), jnp.float32),) * FG)
        field = lax.broadcasted_iota(jnp.int32, (1, N), 1) // B
        scale = jnp.zeros((1, N), jnp.float32)
        for f, peak in enumerate(peaks):
            peak = jnp.max(jnp.max(peak, axis=1, keepdims=True), axis=0, keepdims=True)
            scale = jnp.where(field == f, peak, scale)
        return scale_of(scale * 2.0 ** -11)

    def x_step(grp, scale, lo, hi, before_send=None):
        slot = lax.rem(grp, 2)

        def body(yy, _):
            pieces = []
            for dy in range(2):
                y = yy * 2 + dy
                halves = [stage[slot, c, :, pl.ds(y, 1)].reshape(FG * B, N) for c in range(2)]
                pieces.append(jnp.concatenate(halves, axis=1))
            data = jnp.concatenate(pieces, axis=0)
            rows = 2 * NP * KC
            out = lax.dot_general(fx_ref[lo * rows:hi * rows, :], data, (((1,), (1,)), ((), ())), precision=highest,
                                  preferred_element_type=jnp.float32)
            for dy in range(2):
                for blk in range((hi - lo) * NP * 2):
                    base = (lo * NP + blk // 2) * MSG + blk % 2 * B + yy * 2 + dy
                    xout[pl.ds(base, KC, stride=2 * B), :] = out[blk * KC:(blk + 1) * KC, dy * N:(dy + 1) * N]
            return 0

        lax.fori_loop(0, B // 2, body, 0)
        tail = jnp.broadcast_to(scale, (SC, N)).astype(jnp.bfloat16)
        if before_send is not None:
            before_send()

        def send(j, _):
            t = grp * NJ + j
            place = lax.rem(t, 2 * NJ)

            def pack(r, _):
                rows = pl.ds(pl.multiple_of((j * NP + r) * MSG, MSG), MSG)
                xsend[place, r, :MSG, :] = encode(xout[rows, :], scale)
                xsend[place, r, MSG:, :] = tail
                return 0

            lax.fori_loop(0, NP, pack, 0)
            for d in (2, 3, 1, 0):
                row_copy(t, d).start()
            return 0

        lax.fori_loop(lo, hi, send, 0)

    def row_drained(grp):
        def body(j, _):
            for d in (1, 2, 3):
                row_copy(grp * NJ + j, d).wait_send()
            return 0

        lax.fori_loop(0, NJ, body, 0)

    def y_step(t):
        slot = lax.rem(t, YS)
        arrived(xrecv, xr_sem, t)
        given = [xrecv[t, p, MSG:, :].astype(jnp.float32)[:1] for p in range(NP)]
        scale = scale_of(4.0 * sum(given))

        @pl.when(lax.rem(t, NJ) == 0)
        def _():
            ssend[t // NJ] = jnp.broadcast_to(scale, (SC, N)).astype(jnp.bfloat16)
            for d in (2, 3, 1, 0):
                scale_copy(t // NJ, d).start()

        scale2 = jnp.concatenate([scale, scale], axis=1)

        def body(kk, _):
            cols = []
            for dk in range(2):
                k = kk * 2 + dk
                rows = pl.ds(pl.multiple_of(k * 2 * B, 2 * B), 2 * B)
                cols.append(jnp.concatenate(
                    [decode(xrecv[t, p, rows, :], given[p]) for p in range(NP)],
                    axis=0))
            data = jnp.concatenate(cols, axis=1)
            out = jnp.dot(fy_ref[...], data, precision=highest, preferred_element_type=jnp.float32)
            out = encode(out, scale2)
            for dk in range(2):
                for s in range(NP):
                    for c in range(2):
                        rows = pl.ds(pl.multiple_of(c * KC * B + (kk * 2 + dk) * B, B), B)
                        ysend[slot, s, rows, :] = out[(s * 2 + c) * B:(s * 2 + c + 1) * B, dk * N:(dk + 1) * N]
            return 0

        lax.fori_loop(0, KC // 2, body, 0)
        @pl.when(t < nt - 1)
        def _():
            for d in (2, 3, 1, 0):
                col_copy(t, d).start()

        @pl.when(t == nt - 1)
        def _():
            for d in (1, 2, 3, 0):
                col_copy(t, d).start()


    def z_step(t):
        grp, j = t // NJ, lax.rem(t, NJ)
        @pl.when(j == 0)
        def _():
            arrived(srecv, sr_sem, grp)

        arrived(yrecv, yr_sem, t)
        gain = g_ref[pl.ds(j * KC, KC)].reshape(KC * B, N)
        for f in range(FG):
            parts = z_field(f, [yrecv[t, q] for q in range(NP)], [srecv[grp, q] for q in range(NP)], fz_ref, gain)
            for part, dst in zip(parts, (wr_ref, wi_ref)):
                dst[grp * FG + f, pl.ds(j * KC, KC)] = part

    for grp in range(min(2, ng)):
        for copy in load(grp, grp):
            copy.start()

    barrier = pltpu.get_barrier_semaphore()
    for d in range(1, NP):
        pl.semaphore_signal(barrier, inc=1, device_id={"row": peer(row, d)}, device_id_type=MESH)
        pl.semaphore_signal(barrier, inc=1, device_id={"col": peer(col, d)}, device_id_type=MESH)

    scale0 = row_scale(0)
    x_step(0, scale0, 0, 1, lambda: pl.semaphore_wait(barrier, 2 * (NP - 1)))
    x_step(0, scale0, 1, NJ)
    if ng > 2:
        for copy in load(2, 0):
            copy.start()

    def tick(t, _):
        @pl.when(t >= YS)
        def _():
            for d in (1, 2, 3):
                col_copy(t - YS, d).wait_send()

        y_step(t)

        if ng > 1:
            @pl.when(t == NJ - 3)
            def _():
                x_step(1, row_scale(1), 0, NJ)

        @pl.when(t >= LAG)
        def _():
            z_step(t - LAG)

        if ng > 2:
            @pl.when((lax.rem(t, NJ) == NJ - 1) & (t < (ng - 2) * NJ))
            def _():
                grp = t // NJ
                row_drained(grp)
                x_step(grp + 2, row_scale(grp + 2), 0, NJ)

                @pl.when(grp + 3 < ng)
                def _():
                    for copy in load(grp + 3, lax.rem(grp + 3, 2)):
                        copy.start()

        return 0

    lax.fori_loop(0, nt, tick, 0)

    def drain(t, _):
        z_step(t)
        return 0

    lax.fori_loop(max(nt - LAG, 0), nt - 1, drain, 0)
    arrived(yrecv, yr_sem, nt - 1)
    for q in range(NP):
        code_ref[q] = yrecv[nt - 1, q]
        scale_ref[q] = srecv[ng - 1, q]
    for grp in range(max(ng - 2, 0), ng):
        row_drained(grp)
    for t in range(max(nt - YS, 0), nt):
        for d in (1, 2, 3):
            col_copy(t, d).wait_send()
    for grp in range(ng):
        for d in (1, 2, 3):
            scale_copy(grp, d).wait_send()


def solution(mesh):
    fx, fy, fz = dft_tables()

    def local_forward(u_real, u_imag, g_filter):
        ng = u_real.shape[0] // FG
        nt = ng * NJ
        u_real, u_imag = (jnp.transpose(u, (0, 2, 3, 1)) for u in (u_real, u_imag))
        out = pltpu.VMEM((ng * FG, B, B, N), jnp.float32)
        vmem, anywhere = pl.BlockSpec(memory_space=pltpu.VMEM), pl.BlockSpec(memory_space=pl.ANY)
        flops = 2 * 2 * N * 2 * N * N * B * B // N * ng * FG * 24
        w_real, w_imag, code, scale = pl.pallas_call(
            functools.partial(kernel, ng),
            out_shape=(out, out, pltpu.VMEM((NP, MSG, N), jnp.bfloat16), pltpu.VMEM((NP, SC, N), jnp.bfloat16)),
            in_specs=[vmem] * 4 + [anywhere] * 2,
            out_specs=(vmem,) * 4,
            scratch_shapes=[
                pltpu.VMEM((2, 2, FG, B, B, N), jnp.float32),
                pltpu.VMEM((NP * NJ * MSG, N), jnp.float32),
                pltpu.VMEM((2 * NJ, NP, MSG + SC, N), jnp.bfloat16),
                pltpu.VMEM((nt, NP, MSG + SC, N), jnp.bfloat16),
                pltpu.VMEM((YS, NP, MSG, N), jnp.bfloat16),
                pltpu.VMEM((nt, NP, MSG, N), jnp.bfloat16),
                pltpu.VMEM((ng, SC, N), jnp.bfloat16),
                pltpu.VMEM((ng, NP, SC, N), jnp.bfloat16),
                pltpu.SemaphoreType.DMA((2, 2)),
                pltpu.SemaphoreType.DMA((2 * NJ, NP)),
                pltpu.SemaphoreType.DMA((nt, NP)),
                pltpu.SemaphoreType.DMA((YS, NP)),
                pltpu.SemaphoreType.DMA((nt, NP)),
                pltpu.SemaphoreType.DMA((ng, NP)),
                pltpu.SemaphoreType.DMA((ng, NP)),
            ],
            compiler_params=pltpu.CompilerParams(
                collective_id=0, has_side_effects=True, vmem_limit_bytes=44 << 20),
            cost_estimate=pl.CostEstimate(flops=flops, bytes_accessed=1 << 25, transcendentals=0),
        )(jnp.asarray(fx), jnp.asarray(fy), jnp.asarray(fz), g_filter, u_real, u_imag)
        result = jax.ShapeDtypeStruct((ng * FG, B, B, N), jnp.float32)
        return pl.pallas_call(
            functools.partial(finish, ng),
            out_shape=(result, result),
            in_specs=[vmem] * 6,
            out_specs=(anywhere, anywhere),
            scratch_shapes=[
                pltpu.VMEM((2, FG, KC, B, N), jnp.float32),
                pltpu.SemaphoreType.DMA((2, 2)),
                pltpu.SemaphoreType.DMA((2, FG)),
            ],
            compiler_params=pltpu.CompilerParams(vmem_limit_bytes=16 << 20),
        )(jnp.asarray(fz), g_filter, w_real, w_imag, code, scale)

    field_spec = P("fld", None, "row", "col")
    out_spec = P("fld", "row", "col", None)
    return jax.shard_map(local_forward, mesh=mesh, in_specs=(field_spec, field_spec, P("row", "col", None)),
                         out_specs=(out_spec, out_spec), check_vma=False)
```

```python
import functools
import math

import jax
import jax.numpy as jnp
import numpy as np
from jax import lax
from jax.experimental import pallas as pl
from jax.experimental.pallas import tpu as pltpu
from jax.sharding import PartitionSpec as P

MESH = pl.DeviceIdType.MESH
N = 128
B = 32
NP = 4
FG = 4
KC = 8
NJ = B // KC
MSG = 2 * KC * B
SC = 16
TINY = 2.0 ** -126
LAG = 8
HOLD = 3
YS = LAG + HOLD + 2


def dft_tables():
    idx = np.arange(N)
    ang = 2.0 * np.pi * ((idx[:, None] * idx[None, :]) % N) / N
    cos, sin = np.cos(ang) / math.sqrt(N), np.sin(ang) / math.sqrt(N)
    mat = np.stack([np.stack([cos, sin], 1), np.stack([-sin, cos], 1)])
    fx = mat.reshape(2, NP, NJ, KC, 2 * N).transpose(2, 1, 0, 3, 4).reshape(2 * N, 2 * N)
    fy = mat.reshape(2, NP, B, 2, NP, B).transpose(1, 0, 2, 4, 3, 5).reshape(2 * N, 2 * N)
    fz = mat.transpose(2, 3, 0, 1).reshape(2 * N, 2 * N)
    return fx.astype(np.float32), fy.astype(np.float32), fz.astype(np.float32)


def encode(x, scale):
    v = x * (1.0 / scale)
    p = v * v
    p = p * p
    p = p * p
    return jnp.where(v < 0, -p, p).astype(jnp.bfloat16)


def decode(code, scale):
    y = code.astype(jnp.float32)
    p = jnp.maximum(jnp.abs(y), TINY)
    root = lax.rsqrt(lax.rsqrt(p * lax.rsqrt(p)))
    return jnp.where(y == 0, 0.0, jnp.where(y < 0, -root, root)) * scale


def scale_of(x):
    return jnp.maximum(x, TINY).astype(jnp.bfloat16).astype(jnp.float32)


def take(f, pieces):
    group = lax.broadcasted_iota(jnp.int32, pieces[0].shape, 1) // B
    code = None
    for q, piece in enumerate(pieces):
        if q != f:
            piece = pltpu.roll(piece, (q - f) % NP * B, 1)
        code = piece if code is None else jnp.where(group == q, piece, code)
    return code


def z_field(f, codes, scales, fz_ref, gain):
    half = KC * B
    code = take(f, codes)
    scale = take(f, [s.astype(jnp.float32) for s in scales])[:1]
    data = jnp.concatenate([decode(code[c * half:(c + 1) * half], scale) for c in range(2)], axis=1)
    out = jnp.dot(data, fz_ref[...], precision=lax.Precision.HIGHEST, preferred_element_type=jnp.float32)
    return [(out[:, c * N:(c + 1) * N] * gain).reshape(KC, B, N) for c in range(2)]


def finish(ng, fz_ref, g_ref, wr_ref, wi_ref, code_ref, scale_ref, or_ref, oi_ref, stage, sem, last_sem):
    kx, done = (NJ - 1) * KC, (ng - 1) * FG
    copies = []
    for c, (src, dst) in enumerate(((wr_ref, or_ref), (wi_ref, oi_ref))):
        tail = (pl.ds(done, FG), pl.ds(0, kx))
        copies.append(pltpu.make_async_copy(src.at[tail], dst.at[tail], sem.at[c, 0]))
        if done:
            copies.append(pltpu.make_async_copy(src.at[pl.ds(0, done)], dst.at[pl.ds(0, done)], sem.at[c, 1]))
    for copy in copies:
        copy.start()
    gain = g_ref[kx:].reshape(KC * B, N)
    for f in range(FG):
        parts = z_field(f, [code_ref[q] for q in range(NP)], [scale_ref[q] for q in range(NP)], fz_ref, gain)
        for c, (part, dst) in enumerate(zip(parts, (or_ref, oi_ref))):
            stage[c, f] = part
            copy = pltpu.make_async_copy(stage.at[c, f], dst.at[done + f, pl.ds(kx, KC)], last_sem.at[c, f])
            copy.start()
            copies.append(copy)
    for copy in copies:
        copy.wait()


def kernel(ng, fx_ref, fy_ref, fz_ref, g_ref, ur_ref, ui_ref, wr_ref, wi_ref, code_ref, scale_ref,
           stage, xout, xsend, xrecv, ysend, yrecv, ssend, srecv,
           in_sem, xs_sem, xr_sem, ys_sem, yr_sem, ss_sem, sr_sem):
    nt = ng * NJ
    col, row = lax.axis_index("col"), lax.axis_index("row")
    highest = lax.Precision.HIGHEST

    def peer(me, d):
        return (me, me + 1 - 2 * lax.rem(me, 2), lax.rem(me + 2, NP), NP - 1 - me)[d]

    def load(grp, slot):
        copies = []
        for c, src in enumerate((ur_ref, ui_ref)):
            copies.append(pltpu.make_async_copy(src.at[pl.ds(grp * FG, FG)], stage.at[slot, c], in_sem.at[slot, c]))
        return copies

    def row_copy(t, d):
        dst = peer(row, d)
        src = xsend.at[lax.rem(t, 2 * NJ), dst]
        if d == 0:
            return pltpu.make_async_copy(src, xrecv.at[t, row], xr_sem.at[t, row])
        return pltpu.make_async_remote_copy(
            src, xrecv.at[t, row], xs_sem.at[lax.rem(t, 2 * NJ), d], xr_sem.at[t, row],
            device_id={"row": dst}, device_id_type=MESH)

    def col_copy(t, d):
        dst = peer(col, d)
        src = ysend.at[lax.rem(t, YS), dst]
        if d == 0:
            return pltpu.make_async_copy(src, yrecv.at[t, col], yr_sem.at[t, col])
        return pltpu.make_async_remote_copy(
            src, yrecv.at[t, col], ys_sem.at[lax.rem(t, YS), d], yr_sem.at[t, col],
            device_id={"col": dst}, device_id_type=MESH)

    def scale_copy(grp, d):
        dst = peer(col, d)
        src = ssend.at[grp]
        if d == 0:
            return pltpu.make_async_copy(src, srecv.at[grp, col], sr_sem.at[grp, col])
        return pltpu.make_async_remote_copy(
            src, srecv.at[grp, col], ss_sem.at[grp, d], sr_sem.at[grp, col],
            device_id={"col": dst}, device_id_type=MESH)

    def arrived(buf, sem, t):
        for p in range(NP):
            pltpu.make_async_copy(buf.at[t, p], buf.at[t, p], sem.at[t, p]).wait()

    def row_scale(grp):
        slot = lax.rem(grp, 2)
        for copy in load(grp, slot):
            copy.wait()

        def body(y, peaks):
            blocks = [jnp.abs(stage[slot, :, f, pl.ds(y, 1)]).reshape(2 * B // 8, 8, N) for f in range(FG)]
            return tuple(jnp.maximum(peak, jnp.max(block, axis=0)) for peak, block in zip(peaks, blocks))

        peaks = lax.fori_loop(0, B, body, (jnp.zeros((8, N), jnp.float32),) * FG)
        field = lax.broadcasted_iota(jnp.int32, (1, N), 1) // B
        scale = jnp.zeros((1, N), jnp.float32)
        for f, peak in enumerate(peaks):
            peak = jnp.max(jnp.max(peak, axis=1, keepdims=True), axis=0, keepdims=True)
            scale = jnp.where(field == f, peak, scale)
        return scale_of(scale * 2.0 ** -11)

    def x_step(grp, scale, lo, hi, before_send=None):
        slot = lax.rem(grp, 2)

        def body(yy, _):
            pieces = []
            for dy in range(2):
                y = yy * 2 + dy
                halves = [stage[slot, c, :, pl.ds(y, 1)].reshape(FG * B, N) for c in range(2)]
                pieces.append(jnp.concatenate(halves, axis=1))
            data = jnp.concatenate(pieces, axis=0)
            rows = 2 * NP * KC
            out = lax.dot_general(fx_ref[lo * rows:hi * rows, :], data, (((1,), (1,)), ((), ())), precision=highest,
                                  preferred_element_type=jnp.float32)
            for dy in range(2):
                for blk in range((hi - lo) * NP * 2):
                    base = (lo * NP + blk // 2) * MSG + blk % 2 * B + yy * 2 + dy
                    xout[pl.ds(base, KC, stride=2 * B), :] = out[blk * KC:(blk + 1) * KC, dy * N:(dy + 1) * N]
            return 0

        lax.fori_loop(0, B // 2, body, 0)
        tail = jnp.broadcast_to(scale, (SC, N)).astype(jnp.bfloat16)
        if before_send is not None:
            before_send()

        def send(j, _):
            t = grp * NJ + j
            place = lax.rem(t, 2 * NJ)

            def pack(r, _):
                rows = pl.ds(pl.multiple_of((j * NP + r) * MSG, MSG), MSG)
                xsend[place, r, :MSG, :] = encode(xout[rows, :], scale)
                xsend[place, r, MSG:, :] = tail
                return 0

            lax.fori_loop(0, NP, pack, 0)
            for d in (2, 3, 1, 0):
                row_copy(t, d).start()
            return 0

        lax.fori_loop(lo, hi, send, 0)

    def row_drained(grp):
        def body(j, _):
            for d in (1, 2, 3):
                row_copy(grp * NJ + j, d).wait_send()
            return 0

        lax.fori_loop(0, NJ, body, 0)

    def y_step(t):
        slot = lax.rem(t, YS)
        arrived(xrecv, xr_sem, t)
        given = [xrecv[t, p, MSG:, :].astype(jnp.float32)[:1] for p in range(NP)]
        scale = scale_of(4.0 * sum(given))

        @pl.when(lax.rem(t, NJ) == 0)
        def _():
            ssend[t // NJ] = jnp.broadcast_to(scale, (SC, N)).astype(jnp.bfloat16)
            for d in (2, 3, 1, 0):
                scale_copy(t // NJ, d).start()

        scale2 = jnp.concatenate([scale, scale], axis=1)

        def body(kk, _):
            cols = []
            for dk in range(2):
                k = kk * 2 + dk
                rows = pl.ds(pl.multiple_of(k * 2 * B, 2 * B), 2 * B)
                cols.append(jnp.concatenate(
                    [decode(xrecv[t, p, rows, :], given[p]) for p in range(NP)],
                    axis=0))
            data = jnp.concatenate(cols, axis=1)
            out = jnp.dot(fy_ref[...], data, precision=highest, preferred_element_type=jnp.float32)
            out = encode(out, scale2)
            for dk in range(2):
                for s in range(NP):
                    for c in range(2):
                        rows = pl.ds(pl.multiple_of(c * KC * B + (kk * 2 + dk) * B, B), B)
                        ysend[slot, s, rows, :] = out[(s * 2 + c) * B:(s * 2 + c + 1) * B, dk * N:(dk + 1) * N]
            return 0

        lax.fori_loop(0, KC // 2, body, 0)
        col_copy(t, 0).start()
        at_end = (col == 0) | (col == NP - 1)

        @pl.when(at_end)
        def _():
            col_copy(t, 1).start()

            @pl.when(t >= HOLD)
            def _():
                for d in (2, 3):
                    col_copy(t - HOLD, d).start()

            @pl.when(t == nt - 1)
            def _():
                for late in range(nt - min(HOLD, nt), nt):
                    for d in (2, 3):
                        col_copy(late, d).start()

        @pl.when(jnp.logical_not(at_end))
        def _():
            for d in (2, 3, 1):
                col_copy(t, d).start()

    def z_step(t):
        grp, j = t // NJ, lax.rem(t, NJ)
        @pl.when(j == 0)
        def _():
            arrived(srecv, sr_sem, grp)

        arrived(yrecv, yr_sem, t)
        gain = g_ref[pl.ds(j * KC, KC)].reshape(KC * B, N)
        for f in range(FG):
            parts = z_field(f, [yrecv[t, q] for q in range(NP)], [srecv[grp, q] for q in range(NP)], fz_ref, gain)
            for part, dst in zip(parts, (wr_ref, wi_ref)):
                dst[grp * FG + f, pl.ds(j * KC, KC)] = part

    for grp in range(min(2, ng)):
        for copy in load(grp, grp):
            copy.start()

    barrier = pltpu.get_barrier_semaphore()
    for d in range(1, NP):
        pl.semaphore_signal(barrier, inc=1, device_id={"row": peer(row, d)}, device_id_type=MESH)
        pl.semaphore_signal(barrier, inc=1, device_id={"col": peer(col, d)}, device_id_type=MESH)

    scale0 = row_scale(0)
    x_step(0, scale0, 0, 1, lambda: pl.semaphore_wait(barrier, 2 * (NP - 1)))
    x_step(0, scale0, 1, NJ)
    if ng > 2:
        for copy in load(2, 0):
            copy.start()

    def tick(t, _):
        @pl.when(t >= YS)
        def _():
            for d in (1, 2, 3):
                col_copy(t - YS, d).wait_send()

        y_step(t)

        if ng > 1:
            @pl.when(t == NJ - 3)
            def _():
                x_step(1, row_scale(1), 0, NJ)

        @pl.when(t >= LAG)
        def _():
            z_step(t - LAG)

        if ng > 2:
            @pl.when((lax.rem(t, NJ) == NJ - 1) & (t < (ng - 2) * NJ))
            def _():
                grp = t // NJ
                row_drained(grp)
                x_step(grp + 2, row_scale(grp + 2), 0, NJ)

                @pl.when(grp + 3 < ng)
                def _():
                    for copy in load(grp + 3, lax.rem(grp + 3, 2)):
                        copy.start()

        return 0

    lax.fori_loop(0, nt, tick, 0)

    def drain(t, _):
        z_step(t)
        return 0

    lax.fori_loop(max(nt - LAG, 0), nt - 1, drain, 0)
    arrived(yrecv, yr_sem, nt - 1)
    for q in range(NP):
        code_ref[q] = yrecv[nt - 1, q]
        scale_ref[q] = srecv[ng - 1, q]
    for grp in range(max(ng - 2, 0), ng):
        row_drained(grp)
    for t in range(max(nt - YS, 0), nt):
        for d in (1, 2, 3):
            col_copy(t, d).wait_send()
    for grp in range(ng):
        for d in (1, 2, 3):
            scale_copy(grp, d).wait_send()


def solution(mesh):
    fx, fy, fz = dft_tables()

    def local_forward(u_real, u_imag, g_filter):
        ng = u_real.shape[0] // FG
        nt = ng * NJ
        u_real, u_imag = (jnp.transpose(u, (0, 2, 3, 1)) for u in (u_real, u_imag))
        out = pltpu.VMEM((ng * FG, B, B, N), jnp.float32)
        vmem, anywhere = pl.BlockSpec(memory_space=pltpu.VMEM), pl.BlockSpec(memory_space=pl.ANY)
        flops = 2 * 2 * N * 2 * N * N * B * B // N * ng * FG * 24
        w_real, w_imag, code, scale = pl.pallas_call(
            functools.partial(kernel, ng),
            out_shape=(out, out, pltpu.VMEM((NP, MSG, N), jnp.bfloat16), pltpu.VMEM((NP, SC, N), jnp.bfloat16)),
            in_specs=[vmem] * 4 + [anywhere] * 2,
            out_specs=(vmem,) * 4,
            scratch_shapes=[
                pltpu.VMEM((2, 2, FG, B, B, N), jnp.float32),
                pltpu.VMEM((NP * NJ * MSG, N), jnp.float32),
                pltpu.VMEM((2 * NJ, NP, MSG + SC, N), jnp.bfloat16),
                pltpu.VMEM((nt, NP, MSG + SC, N), jnp.bfloat16),
                pltpu.VMEM((YS, NP, MSG, N), jnp.bfloat16),
                pltpu.VMEM((nt, NP, MSG, N), jnp.bfloat16),
                pltpu.VMEM((ng, SC, N), jnp.bfloat16),
                pltpu.VMEM((ng, NP, SC, N), jnp.bfloat16),
                pltpu.SemaphoreType.DMA((2, 2)),
                pltpu.SemaphoreType.DMA((2 * NJ, NP)),
                pltpu.SemaphoreType.DMA((nt, NP)),
                pltpu.SemaphoreType.DMA((YS, NP)),
                pltpu.SemaphoreType.DMA((nt, NP)),
                pltpu.SemaphoreType.DMA((ng, NP)),
                pltpu.SemaphoreType.DMA((ng, NP)),
            ],
            compiler_params=pltpu.CompilerParams(
                collective_id=0, has_side_effects=True, vmem_limit_bytes=46 << 20),
            cost_estimate=pl.CostEstimate(flops=flops, bytes_accessed=1 << 25, transcendentals=0),
        )(jnp.asarray(fx), jnp.asarray(fy), jnp.asarray(fz), g_filter, u_real, u_imag)
        result = jax.ShapeDtypeStruct((ng * FG, B, B, N), jnp.float32)
        return pl.pallas_call(
            functools.partial(finish, ng),
            out_shape=(result, result),
            in_specs=[vmem] * 6,
            out_specs=(anywhere, anywhere),
            scratch_shapes=[
                pltpu.VMEM((2, FG, KC, B, N), jnp.float32),
                pltpu.SemaphoreType.DMA((2, 2)),
                pltpu.SemaphoreType.DMA((2, FG)),
            ],
            compiler_params=pltpu.CompilerParams(vmem_limit_bytes=16 << 20),
        )(jnp.asarray(fz), g_filter, w_real, w_imag, code, scale)

    field_spec = P("fld", None, "row", "col")
    out_spec = P("fld", "row", "col", None)
    return jax.shard_map(local_forward, mesh=mesh, in_specs=(field_spec, field_spec, P("row", "col", None)),
                         out_specs=(out_spec, out_spec), check_vma=False)
```
